32 devices in a mesh: dp: 8 (over z, x), cent: 4 (over y, core).
Axes of the slice: x: 2, y: 2, z: 4, core: 2. Of those that a mesh axis runs over, the one named last changes fastest.
Arguments:
- documents: bfloat16 [16384, 2048], P(('dp', 'cent')), may hold values from -6 to 6
- assigned: int32 [16384], P(('dp', 'cent')), may hold values from 0 to 12287, as said below
- centroids: bfloat16 [12288, 2048], P(('dp', 'cent')), may hold values from -6 to 6
- owner_slot: int32 [12288], replicated, may hold values from 0 to 12287, as said below
Outputs:
- prototypicality: float32 [16384], P(('dp', 'cent'))
- redundancy: float32 [16384], P(('dp', 'cent'))
- cluster_stats: float32 [3, 12288], P(None, ('dp', 'cent'))
The draws below stay inside these ranges and needn't reach their ends.
Inputs may be any that keep to these rules, and one draw needn't show every extreme that they name: `owner_slot`: A permutation of the cluster numbers. `assigned`: of the 512 documents of one device, at most 32 have a slot in any one owner's block of 384 slots, and at most 80 have slots with the owners that share one dp index; in every draw some device reaches 80, and one owner receives exactly 32 from every device.
All inputs are finite; a program needn't handle non-finite values.
Results may differ from the reference program's by a relative error of at most 0.0003.
Values may be sent and summed in bfloat16 or wider, within the bound.
A program may use at most 64 MiB of HBM per device.

```python
import jax
import jax.numpy as jnp
from jax import lax

D = 2048
DOC_DEV = 512
CL_DEV = 384
DOCS = 16384
CLUSTERS = 12288
CAP = 32
GCAP = 80
N_CENT = 4
DEVICES = 32


def slot_permutation(key):
    return jax.random.permutation(jax.random.fold_in(key, 11), CLUSTERS).astype(jnp.int32)


def draw_owner_slot(key, part):
    return slot_permutation(key)


def draw_assigned(key, part):
    permuted = slot_permutation(key)
    inverse = jnp.zeros((CLUSTERS,), jnp.int32).at[permuted].set(jnp.arange(CLUSTERS, dtype=jnp.int32))
    base = jax.random.fold_in(key, 23)
    key_forced = jax.random.fold_in(base, 1)
    key_favour = jax.random.fold_in(base, 2)
    key_ticket = jax.random.fold_in(base, 3)
    key_choose = jax.random.fold_in(base, 4)
    key_shuffle = jax.random.fold_in(base, 5)
    key_local = jax.random.fold_in(base, 6)
    row_count = DEVICES // N_CENT
    per_row = N_CENT * CAP
    forced = jax.random.randint(key_forced, (), 0, DEVICES, dtype=jnp.int32)
    forced_row = forced // N_CENT
    forced_col = forced % N_CENT
    row_ids = jnp.arange(row_count, dtype=jnp.int32)[None, :]
    favour = jax.random.randint(key_favour, (DEVICES, row_count), 0, N_CENT, dtype=jnp.int32)
    favour = jnp.where(row_ids == forced_row, forced_col, favour)
    ticket_ids = jnp.arange(per_row, dtype=jnp.int32)
    ticket_col = ticket_ids // CAP
    noise = jax.random.randint(key_ticket, (DEVICES, row_count, per_row), 0, 1 << 19, dtype=jnp.int32)
    boost = jnp.where(ticket_col[None, None, :] == favour[:, :, None], 1 << 29, 0).astype(jnp.int32)
    score = noise * per_row + ticket_ids[None, None, :] + boost
    kept = jnp.argsort(-score, axis=-1)[:, :, :GCAP].astype(jnp.int32)
    kept_owner = row_ids[:, :, None] * N_CENT + kept // CAP
    kept_owner = kept_owner.reshape(DEVICES, row_count * GCAP)
    pool = row_count * GCAP
    pool_ids = jnp.arange(pool, dtype=jnp.int32)
    pool_row = pool_ids // GCAP
    noise_two = jax.random.randint(key_choose, (DEVICES, pool), 0, 1 << 19, dtype=jnp.int32)
    boost_two = jnp.where(pool_row == forced_row, 1 << 29, 0).astype(jnp.int32)
    score_two = noise_two * pool + pool_ids[None, :] + boost_two[None, :]
    chosen = jnp.argsort(-score_two, axis=-1)[:, :DOC_DEV].astype(jnp.int32)
    chosen_owner = jnp.take_along_axis(kept_owner, chosen, axis=1)
    noise_three = jax.random.randint(key_shuffle, (DEVICES, DOC_DEV), 0, 1 << 19, dtype=jnp.int32)
    score_three = noise_three * DOC_DEV + jnp.arange(DOC_DEV, dtype=jnp.int32)[None, :]
    shuffled = jnp.argsort(score_three, axis=-1).astype(jnp.int32)
    final_owner = jnp.take_along_axis(chosen_owner, shuffled, axis=1)
    local_draws = jax.random.randint(key_local, (3, DEVICES, DOC_DEV), 0, CL_DEV, dtype=jnp.int32)
    local_ids = jnp.min(local_draws, axis=0)
    slot_ids = final_owner * CL_DEV + local_ids
    return inverse[slot_ids.reshape(DOCS)]


def block_levels(stream_key, extent, pieces, smallest, high):
    gain, own = 1.0, jax.random.fold_in(stream_key, 6)
    for dim, shards_of in pieces:
        steps = jnp.exp(jax.random.uniform(jax.random.fold_in(own, dim), (shards_of,), jnp.float32, smallest / len(pieces), high / len(pieces)))
        gain = gain * jnp.repeat(steps, extent[dim] // shards_of).reshape([-1 if axis == dim else 1 for axis in range(len(extent))])
    return gain


def normal_values(key, shape, scale, reach, cuts=(), held_as=jnp.bfloat16):
    entries = jax.random.normal(key, shape, jnp.float32) * scale
    if len(cuts) > 0:
        entries = block_levels(key, shape, cuts, -0.22, 0.18) * entries
    return jnp.clip(entries, min=-reach, max=reach).astype(held_as)


def setup_inputs(seed: int = 0) -> dict:
    key_list = jax.random.split(jax.random.key(seed), 5)
    documents = normal_values(key_list[0], (DOCS, D), 1.0, 6.0, ((0, 32),))
    assigned = draw_assigned(jax.random.fold_in(key_list[4], 71), 0)
    centroids = normal_values(key_list[2], (CLUSTERS, D), 1.0, 6.0, ((0, 32),))
    owner_slot = draw_owner_slot(jax.random.fold_in(key_list[4], 71), 0)
    return dict(documents=documents, assigned=assigned, centroids=centroids, owner_slot=owner_slot)


def reference(documents, assigned, centroids, owner_slot):
    slot_ids = owner_slot[assigned]
    owner_ids = slot_ids // CL_DEV
    cent_sq = lax.optimization_barrier(jnp.sum(jnp.square(centroids.astype(jnp.float32)), axis=1))

    def block_sim(packed):
        doc_block, slot_block = packed
        doc_rows = doc_block.astype(jnp.float32)
        cent_rows = centroids[slot_block].astype(jnp.float32)
        cross_dot = lax.optimization_barrier(jnp.sum(doc_rows * cent_rows, axis=1))
        self_sq = lax.optimization_barrier(jnp.sum(doc_rows * doc_rows, axis=1))
        similar = cross_dot * lax.rsqrt(self_sq + 1.0) * lax.rsqrt(cent_sq[slot_block] + 1.0)
        return (similar, self_sq)
    similarity, self_sq = lax.map(block_sim, (documents.reshape(DEVICES, DOC_DEV, D), slot_ids.reshape(DEVICES, DOC_DEV)))
    similarity = similarity.reshape(DOCS)
    self_sq = self_sq.reshape(DOCS)
    counts = jax.ops.segment_sum(jnp.ones((DOCS,), jnp.float32), slot_ids, num_segments=CLUSTERS)
    totals = jax.ops.segment_sum(similarity, slot_ids, num_segments=CLUSTERS)
    squares = jax.ops.segment_sum(similarity * similarity, slot_ids, num_segments=CLUSTERS)
    cluster_stats = jnp.stack([counts, totals, squares])
    count_floor = jnp.maximum(counts, 1.0)
    mean_sim = totals / count_floor
    variance = jnp.maximum(squares / count_floor - mean_sim * mean_sim, 0.0)
    prototypicality = (mean_sim[slot_ids] - similarity) / jnp.sqrt(variance[slot_ids] + 1.0 / D)
    owner_grid = owner_ids.reshape(DEVICES, DOC_DEV)
    is_owner = (owner_grid[:, :, None] == jnp.arange(DEVICES, dtype=jnp.int32)[None, None, :]).astype(jnp.int32)
    rank_ids = lax.optimization_barrier(jnp.sum((jnp.cumsum(is_owner, axis=1) - 1) * is_owner, axis=2)).astype(jnp.int32)
    source_ids = jnp.arange(DEVICES, dtype=jnp.int32)[:, None]
    position = owner_grid * (DEVICES * CAP) + source_ids * CAP + rank_ids
    member_table = jnp.full((DEVICES * DEVICES * CAP,), DOCS, jnp.int32)
    member_table = member_table.at[position.reshape(-1)].set(jnp.arange(DOCS, dtype=jnp.int32))
    member_table = member_table.reshape(DEVICES, DEVICES * CAP)
    inverse_norm = lax.rsqrt(self_sq + 1.0)
    slot_count = DEVICES * CAP
    not_self = jnp.arange(slot_count, dtype=jnp.int32)[:, None] != jnp.arange(slot_count, dtype=jnp.int32)[None, :]

    def owner_redundancy(members):
        is_live = members < DOCS
        safe_ids = jnp.minimum(members, DOCS - 1)
        doc_rows = documents[safe_ids].astype(jnp.float32)
        gram_block = jnp.dot(doc_rows, doc_rows.T, precision=lax.Precision.HIGHEST)
        row_scale = jnp.where(is_live, inverse_norm[safe_ids], 0.0)
        cosine = gram_block * row_scale[:, None] * row_scale[None, :]
        cluster_tag = jnp.where(is_live, slot_ids[safe_ids], -1)
        same_cluster = (cluster_tag[:, None] == cluster_tag[None, :]) & is_live[:, None] & not_self
        return jnp.sqrt(jnp.float32(D)) * lax.optimization_barrier(jnp.max(jnp.where(same_cluster, cosine, 0.0), axis=1))
    redundant = lax.map(owner_redundancy, member_table)
    redundancy = jnp.zeros((DOCS,), jnp.float32).at[member_table.reshape(-1)].set(redundant.reshape(-1), mode='drop')
    return (prototypicality, redundancy, cluster_stats)
```

```python
import functools
import math

import jax
import jax.numpy as jnp
from jax import lax
from jax.experimental import pallas as pl
from jax.experimental.pallas import tpu as pltpu
from jax.sharding import PartitionSpec as P

F32 = jnp.float32
BF16 = jnp.bfloat16
LANES = 128
SUB = 8


def round_up(value, unit):
    return -(-value // unit) * unit


def each(low, high, body):
    if high - low <= 8:
        for step in range(low, high):
            body(step)
    else:
        lax.fori_loop(low, high, lambda step, carry: (body(step), carry)[1], 0)


def iota(shape, dim):
    return lax.broadcasted_iota(jnp.int32, shape, dim)


def mm(left, right):
    return lax.dot_general(left, right, (((1,), (0,)), ((), ())), preferred_element_type=F32)


def mm_t(left, right):
    return lax.dot_general(left, right, (((1,), (1,)), ((), ())), preferred_element_type=F32)


def one_hot(condition):
    return jnp.where(condition, 1.0, 0.0).astype(BF16)


def split3(value):
    high = value.astype(BF16)
    rest = value - high.astype(F32)
    mid = rest.astype(BF16)
    low = (rest - mid.astype(F32)).astype(BF16)
    return high, mid, low


def kernel(
    dims,
    docs_hbm,
    assigned_hbm,
    cent_hbm,
    table_hbm,
    out_ref,
    docs_ref,
    assigned_ref,
    table_ref,
    all_buf,
    send_buf,
    chunk_buf,
    code_send,
    code_recv,
    fwd_buf,
    tbl_send,
    tbl_recv,
    res_send,
    res_recv,
    res_rows,
    tag_row,
    tag_mat,
    inv_row,
    inv_mat,
    sim_row,
    best_row,
    best_mat,
    cent_mat,
    gram_acc,
    stats_ref,
    in_sem,
    a_send,
    a_recv,
    m_send,
    m_recv,
    f_send,
    f_recv,
    t_send,
    t_recv,
    r_send,
    r_recv,
):
    R, C, K, Q, PIECES = dims
    O = R * C
    CK = C * K
    L, D = docs_ref.shape
    S = cent_hbm.shape[0]
    T = table_ref.shape[0]
    W = D // PIECES
    QP = code_send.shape[2]
    small = R <= 8
    row_me = lax.axis_index("dp")
    col_me = lax.axis_index("cent")
    own = row_me * C + col_me

    bits = []
    while 2 ** len(bits) < R:
        bits.append(lax.rem(lax.div(row_me, 2 ** len(bits)), 2))
    col_of = [col_me] + [lax.rem(col_me + d, C) for d in range(1, C)]

    def row_of(t):
        total = 0
        for i, bit in enumerate(bits):
            if isinstance(t, int):
                total = total + (1 - bit if (t >> i) & 1 else bit) * 2**i
            else:
                total = total + lax.rem(bit + lax.div(t, 2**i), 2) * 2**i
        return total

    def all_peers(body):
        def at_row(t):
            r = row_of(t)
            for d in range(C):
                body(t, r, d)

        each(1, R, at_row)
        for d in range(1, C):
            body(0, row_me, d)

    def where_is(r, c):
        return {"dp": r, "cent": c}

    def remote(src, dst, send, recv, r, c):
        return pltpu.make_async_remote_copy(
            src_ref=src,
            dst_ref=dst,
            send_sem=send,
            recv_sem=recv,
            device_id=where_is(r, c),
            device_id_type=pl.DeviceIdType.MESH,
        )

    barrier = pltpu.get_barrier_semaphore()

    def greet(t, r, d):
        pl.semaphore_signal(
            barrier, inc=1, device_id=where_is(r, col_of[d]), device_id_type=pl.DeviceIdType.MESH
        )

    all_peers(greet)

    cent_rows = all_buf.at[pl.ds(0, S), :]
    loads = [
        pltpu.make_async_copy(assigned_hbm, assigned_ref, in_sem.at[0]),
        pltpu.make_async_copy(table_hbm, table_ref, in_sem.at[1]),
        pltpu.make_async_copy(docs_hbm, docs_ref, in_sem.at[2]),
        pltpu.make_async_copy(cent_hbm, cent_rows, in_sem.at[3]),
    ]
    for load in loads:
        load.start()
    loads[0].wait()
    loads[1].wait()

    assigned = assigned_ref[...]
    high = lax.shift_right_logical(assigned, 7)
    low = jnp.bitwise_and(assigned, 127)
    table = table_ref[...]
    pick = one_hot(iota((T, L), 0) == high)
    looked = jnp.zeros((LANES, L), F32)
    shift = 0
    while 2**shift < O * S:
        digit = jnp.bitwise_and(lax.shift_right_logical(table, shift), 255)
        looked = looked + float(2**shift) * lax.dot_general(
            digit.astype(F32).astype(BF16), pick, (((0,), (0,)), ((), ())), preferred_element_type=F32
        )
        shift += 8
    slot = jnp.sum(jnp.where(iota((LANES, L), 0) == low, looked, 0.0), axis=0, keepdims=True)
    owner = jnp.floor((slot + 0.5) * (1.0 / S))
    row = jnp.floor((owner + 0.5) * (1.0 / C))
    owner_i = owner.astype(jnp.int32)
    row_i = row.astype(jnp.int32)
    cent_i = owner_i - row_i * C
    is_owner = jnp.where(iota((O, L), 0) == owner_i, 1.0, 0.0)
    is_row = jnp.where(iota((R, L), 0) == row_i, 1.0, 0.0)
    earlier = one_hot(iota((L, L), 0) < iota((L, L), 1))
    ranks = mm(jnp.concatenate([is_owner, is_row], axis=0).astype(BF16), earlier)
    rank_owner = jnp.sum(ranks[:O] * is_owner, axis=0, keepdims=True)
    rank_row = jnp.sum(ranks[O:] * is_row, axis=0, keepdims=True)
    position = jnp.bitwise_xor(row_i, row_me) * Q + rank_row.astype(jnp.int32)
    rank_i = rank_owner.astype(jnp.int32)

    ahead = cent_i - col_me
    ahead = jnp.where(ahead < 0, ahead + C, ahead)
    behind = jnp.where(ahead == 0, 0, C - ahead)
    lane_i = behind * K + rank_i
    code = ((ahead * K + rank_i) + 1).astype(F32).astype(BF16)
    code8 = jnp.broadcast_to(code, (SUB, L))
    is_lane = one_hot(iota((LANES, L), 0) == lane_i)

    tag = slot - owner * S + 1.0
    tag_hi = jnp.floor(tag * (1.0 / 128.0))
    tag_lo = tag - tag_hi * 128.0
    tags = mm_t(jnp.concatenate([is_owner * tag_hi, is_owner * tag_lo], axis=0).astype(BF16), is_lane)
    tags = 128.0 * tags[:O] + tags[O:]
    for o in range(O):
        tbl_send[o] = tags[o : o + 1, :]

    def mark(t):
        line = mm_t(code8, one_hot(iota((QP, L), 0) + t * Q == jnp.where(position < (t + 1) * Q, position, -1)))
        code_send[t] = line[0:1, :]

    each(0, R, mark)

    def row_copy(t, p):
        at = pl.ds(p * W, W)
        return remote(
            send_buf.at[t, :, at], chunk_buf.at[t, :, at], a_send.at[t, p], a_recv.at[t, p], row_of(t), col_me
        )

    def code_copy(t):
        return remote(code_send.at[t], code_recv.at[t], m_send.at[t], m_recv.at[t], row_of(t), col_me)

    def tbl_copy(t, r, d):
        return remote(
            tbl_send.at[r * C + col_of[d]],
            tbl_recv.at[t * C + (C - d) % C],
            t_send.at[t * C + d],
            t_recv.at[t * C + (C - d) % C],
            r,
            col_of[d],
        )

    def tbl_arrival(t, r, d):
        return remote(
            tbl_send.at[r * C + col_of[d]],
            tbl_recv.at[t * C + d],
            t_send.at[t * C + d],
            t_recv.at[t * C + d],
            r,
            col_of[d],
        )

    def start_rows(t):
        for p in range(PIECES):
            row_copy(t, p).start()

    def choose(ts):
        wanted = [one_hot(iota((Q, L), 0) + t * Q == position) for t in ts]
        found = mm(jnp.concatenate(wanted, axis=0), docs_ref[...]).astype(BF16)
        for i, t in enumerate(ts):
            send_buf[t] = found[i * Q : (i + 1) * Q]

    def first_sends():
        pl.semaphore_wait(barrier, O - 1)
        each(1, R, lambda t: code_copy(t).start())
        all_peers(lambda t, r, d: tbl_copy(t, r, d).start())

    loads[2].wait()
    if R == 8:
        inner = lax.rem(bits[-1] + bits[-2], 2) == 1
        far = R // 2
        choose([far, 2])
        first_sends()

        @pl.when(inner)
        def _():
            start_rows(far)

        start_rows(2)
        choose([3, 1])
        start_rows(3)

        @pl.when(jnp.logical_not(inner))
        def _():
            start_rows(far)

        start_rows(1)
        choose([5, 6])
        start_rows(5)
        start_rows(6)
        choose([7, 0])
        start_rows(7)
    else:
        first_sends()
        group = max(1, R // 2)
        for first in range(0, R, group):
            wanted = one_hot(iota((group * Q, L), 0) + first * Q == position)
            send_buf[first : first + group] = (
                mm(wanted, docs_ref[...]).astype(BF16).reshape(group, Q, D)
            )
            each(max(first, 1), first + group, start_rows)
    tbl_recv[0] = tbl_send[own]

    def rows_at(t, block=0, count=None):
        return pl.ds(S + t * CK + block * K, CK if count is None else count)

    def fwd_copy(t, d, p):
        at = pl.ds(p * W, W)
        return remote(
            fwd_buf.at[t, d - 1, :, at],
            all_buf.at[rows_at(t, C - d, K), at],
            f_send.at[t, d, p],
            f_recv.at[t, C - d, p],
            row_me,
            col_of[d],
        )

    def fwd_arrival(t, d, p):
        at = pl.ds(p * W, W)
        return remote(
            fwd_buf.at[t, d - 1, :, at],
            all_buf.at[rows_at(t, d, K), at],
            f_send.at[t, d, p],
            f_recv.at[t, d, p],
            row_me,
            col_of[d],
        )

    def relay(t, p, mine=False):
        if not mine:
            row_copy(t, p).wait_recv()
        at = pl.ds(p * W, W)
        line = (code_send if mine else code_recv)[t][:, :Q].astype(jnp.int32)
        wanted = one_hot(iota((CK, Q), 0) + 1 == line)
        found = mm(wanted, (send_buf if mine else chunk_buf)[t, :, at]).astype(BF16)
        fwd_buf[t, :, :, at] = found[K:].reshape(C - 1, K, W)
        for d in range(1, C):
            fwd_copy(t, d, p).start()
        all_buf[rows_at(t, 0, K), at] = found[:K]

    for p in range(PIECES):
        relay(0, p, True)

    loads[3].wait()
    norm = jnp.zeros((S, LANES), F32)
    for part in range(0, D, LANES):
        block = all_buf[0:S, part : part + LANES].astype(F32)
        norm = norm + block * block
    cent_mat[...] = jnp.broadcast_to(
        lax.rsqrt(jnp.sum(norm, axis=1, keepdims=True) + 1.0), cent_mat.shape
    )

    all_peers(lambda t, r, d: tbl_arrival(t, r, d).wait_recv())

    eye = iota((CK, CK), 0) == iota((CK, CK), 1)

    def spread(t):
        line = tbl_recv[t * C]
        for c in range(1, C):
            line = line + tbl_recv[t * C + c]
        line = line[:, :CK]
        tag_row[t] = line
        tag_mat[t] = jnp.broadcast_to(
            jnp.sum(jnp.where(eye, line, 0.0), axis=1, keepdims=True), (CK, CK)
        )
        best_mat[t] = jnp.zeros((CK, CK), F32)

    each(0, R, spread)
    stats_ref[...] = jnp.zeros(stats_ref.shape, F32)

    def member_of(t):
        return (iota((S, CK), 0) + 1).astype(F32) == tag_row[t]

    def self_block(t, gram):
        diag = jnp.where(eye, gram, 0.0)
        row_scale = lax.rsqrt(jnp.sum(diag, axis=0, keepdims=True) + 1.0)
        col_scale = lax.rsqrt(jnp.sum(diag, axis=1, keepdims=True) + 1.0)
        inv_row[t] = row_scale
        inv_mat[t] = jnp.broadcast_to(col_scale, (CK, CK))
        line = jnp.where(tag_row[t] > 0.0, tag_row[t], -1.0)
        same = (tag_mat[t] == line) & jnp.logical_not(eye)
        best = jnp.max(jnp.where(same, gram * col_scale, 0.0), axis=0, keepdims=True)
        return row_scale, line, best

    def other_block(u, gram, row_scale, line, best):
        same = tag_mat[u] == line
        best_mat[u] = jnp.maximum(best_mat[u], jnp.where(same, gram * row_scale, 0.0))
        return jnp.maximum(
            best, jnp.max(jnp.where(same, gram * inv_mat[u], 0.0), axis=0, keepdims=True)
        )

    def cross_block(t, cross, row_scale):
        member = member_of(t)
        similarity = row_scale * jnp.sum(
            jnp.where(member, cross * cent_mat[...], 0.0), axis=0, keepdims=True
        )
        sim_row[t] = similarity
        lines = [jnp.ones((1, CK), BF16), *split3(similarity), *split3(similarity * similarity)]
        lines = jnp.concatenate(
            [line.astype(F32) for line in lines] + [jnp.zeros((1, CK), F32)], axis=0
        )
        stats_ref[...] += mm_t(lines.astype(BF16), one_hot(member))

    def settle(t, read):
        row_scale, line, best = self_block(t, read(S + t * CK, CK))
        for u in range(t):
            best = other_block(u, read(S + u * CK, CK), row_scale, line, best)
        best_row[t] = best
        cross_block(t, read(0, S), row_scale)

    def arrivals(t, p):
        for d in range(1, C):
            fwd_arrival(t, d, p).wait_recv()

    def absorb(t):
        for p in range(PIECES):
            arrivals(t, p)
        gram_acc[0 : S + (t + 1) * CK] = mm_t(all_buf[0 : S + (t + 1) * CK, :], all_buf[rows_at(t), :])
        settle(t, lambda start, count: gram_acc[start : start + count])

    def absorb_piece(t, p):
        arrivals(t, p)
        at = pl.ds(p * W, W)
        rows = S + (t + 1) * CK
        part = mm_t(all_buf[0:rows, at], all_buf[rows_at(t), at])
        gram_acc[0:rows] = part if p == 0 else gram_acc[0:rows] + part

    def absorb_any(t):
        for p in range(PIECES):
            arrivals(t, p)
        mine = all_buf[rows_at(t), :]
        row_scale, line, best = self_block(t, mm_t(mine, mine))

        def pair(u, best):
            return other_block(u, mm_t(all_buf[rows_at(u), :], mine), row_scale, line, best)

        best_row[t] = lax.fori_loop(0, t, pair, best)
        cross_block(t, mm_t(all_buf[0:S, :], mine), row_scale)

    def relay_all(t):
        code_copy(t).wait_recv()
        for p in range(PIECES):
            relay(t, p)

    if small:
        done = 0
        for t in range(1, R - 1):
            relay_all(t)
            while done < (t + 1 if t == R - 3 else t):
                absorb(done)
                done += 1
        last = R - 1
        code_copy(last).wait_recv()
        half = PIECES // 2
        for p in range(half):
            relay(last, p)
        while done < last:
            absorb(done)
            done += 1
        for p in range(half, PIECES):
            relay(last, p)
            absorb_piece(last, p - half)
        for p in range(PIECES - half, PIECES):
            absorb_piece(last, p)
        settle(last, lambda start, count: gram_acc[start : start + count])
    else:

        def advance(t, carry):
            relay_all(t)
            absorb_any(t - 1)
            return carry

        lax.fori_loop(1, R, advance, 0)
        absorb_any(R - 1)

    stats = stats_ref[...]
    count = stats[0:1]
    total = stats[1:2] + stats[2:3] + stats[3:4]
    square = stats[4:5] + stats[5:6] + stats[6:7]
    floor = jnp.maximum(count, 1.0)
    mean = total / floor
    variance = jnp.maximum(square / floor - mean * mean, 0.0)
    spread_inv = 1.0 / jnp.sqrt(variance + 1.0 / D)
    wanted = [line.astype(F32) for line in (*split3(mean), *split3(spread_inv))]
    wanted = jnp.concatenate(wanted + [jnp.zeros((2, S), F32)], axis=0).astype(BF16)

    def res_copy(t, r, d):
        return remote(
            res_send.at[t], res_recv.at[own], r_send.at[t * C + d], r_recv.at[own], r, col_of[d]
        )

    def res_arrival(t, r, d):
        o = r * C + col_of[d]
        return remote(res_send.at[t], res_recv.at[o], r_send.at[t * C + d], r_recv.at[o], r, col_of[d])

    def finish(t):
        found = mm(wanted, one_hot(member_of(t)))
        centre = found[0:1] + found[1:2] + found[2:3]
        width = found[3:4] + found[4:5] + found[5:6]
        proto = (centre - sim_row[t]) * width
        column = jnp.max(best_mat[t], axis=1, keepdims=True)
        flat = jnp.max(jnp.where(eye, column, 0.0), axis=0, keepdims=True)
        redundant = jnp.maximum(flat, best_row[t]) * inv_row[t] * math.sqrt(D)
        res_send[t, 0:1, :CK] = proto
        res_send[t, 1:2, :CK] = redundant

    if CK < LANES:
        res_send[...] = jnp.zeros(res_send.shape, F32)

    def deliver(t):
        finish(t)
        r = row_of(t)
        for d in range(C):
            res_copy(t, r, d).start()

    if small:
        for t in range(R - 1, 0, -1):
            deliver(t)
    else:
        each(1, R, deliver)
    finish(0)
    for d in range(1, C):
        res_copy(0, row_me, d).start()
    res_recv[own] = res_send[0]
    out_ref[2:3, :S] = count
    out_ref[3:4, :S] = total
    out_ref[4:5, :S] = square

    def drain(t):
        code_copy(t).wait_send()
        for p in range(PIECES):
            row_copy(t, p).wait_send()

    each(1, R, drain)

    def drain_fwd(t):
        for d in range(1, C):
            for p in range(PIECES):
                fwd_copy(t, d, p).wait_send()

    each(0, R, drain_fwd)

    def drain_small(t, r, d):
        tbl_copy(t, r, d).wait_send()
        res_copy(t, r, d).wait_send()

    all_peers(drain_small)
    all_peers(lambda t, r, d: res_arrival(t, r, d).wait_recv())

    for o in range(O):
        pair = res_recv[o]
        res_rows[o : o + 1, :] = pair[0:1]
        res_rows[O + o : O + o + 1, :] = pair[1:2]
    parts = jnp.concatenate([line.astype(F32) for line in split3(res_rows[...])], axis=0)
    found = mm(parts.astype(BF16), is_lane)
    found = found[: 2 * O] + found[2 * O : 4 * O] + found[4 * O :]
    mask = iota((O, L), 0) == owner_i
    out_ref[0:1, :L] = jnp.sum(jnp.where(mask, found[:O], 0.0), axis=0, keepdims=True)
    out_ref[1:2, :L] = jnp.sum(jnp.where(mask, found[O:], 0.0), axis=0, keepdims=True)


def local(documents, assigned, centroids, owner_slot):
    L, D = documents.shape
    S = centroids.shape[0]
    R = lax.axis_size("dp")
    C = lax.axis_size("cent")
    O = R * C
    pair_cap = 2 * L // O
    row_cap = 5 * C * pair_cap // 8
    K = round_up(pair_cap, 16)
    Q = round_up(row_cap, 16)
    CK = C * K
    QP = round_up(Q, LANES)
    pieces = 4 if R <= 8 else 1
    T = owner_slot.shape[0] // LANES
    hbm = pl.BlockSpec(memory_space=pl.ANY)
    dma = pltpu.SemaphoreType.DMA
    packed = pl.pallas_call(
        functools.partial(kernel, (R, C, K, Q, pieces)),
        name="cluster_exchange",
        out_shape=jax.ShapeDtypeStruct((SUB, max(L, S)), F32),
        in_specs=[hbm] * 4,
        out_specs=pl.BlockSpec(memory_space=pltpu.VMEM),
        scratch_shapes=[
            pltpu.VMEM((L, D), BF16),
            pltpu.VMEM((1, L), jnp.int32),
            pltpu.VMEM((T, LANES), jnp.int32),
            pltpu.VMEM((S + R * CK, D), BF16),
            pltpu.VMEM((R, Q, D), BF16),
            pltpu.VMEM((R, Q, D), BF16),
            pltpu.VMEM((R, 1, QP), F32),
            pltpu.VMEM((R, 1, QP), F32),
            pltpu.VMEM((R, C - 1, K, D), BF16),
            pltpu.VMEM((O, 1, LANES), F32),
            pltpu.VMEM((O, 1, LANES), F32),
            pltpu.VMEM((R, 2, LANES), F32),
            pltpu.VMEM((O, 2, LANES), F32),
            pltpu.VMEM((2 * O, LANES), F32),
            pltpu.VMEM((R, 1, CK), F32),
            pltpu.VMEM((R, CK, CK), F32),
            pltpu.VMEM((R, 1, CK), F32),
            pltpu.VMEM((R, CK, CK), F32),
            pltpu.VMEM((R, 1, CK), F32),
            pltpu.VMEM((R, 1, CK), F32),
            pltpu.VMEM((R, CK, CK), F32),
            pltpu.VMEM((S, CK), F32),
            pltpu.VMEM((S + R * CK if R <= 8 else SUB, CK), F32),
            pltpu.VMEM((SUB, S), F32),
            dma((4,)),
            dma((R, pieces)),
            dma((R, pieces)),
            dma((R,)),
            dma((R,)),
            dma((R, C, pieces)),
            dma((R, C, pieces)),
            dma((O,)),
            dma((O,)),
            dma((O,)),
            dma((O,)),
        ],
        compiler_params=pltpu.CompilerParams(
            collective_id=0, has_side_effects=True, vmem_limit_bytes=62 * 1024 * 1024
        ),
    )(
        documents,
        assigned.reshape(1, L),
        centroids,
        owner_slot.reshape(-1, LANES),
    )
    return packed[0, :L], packed[1, :L], packed[2:5, :S]


def solution(mesh):
    in_specs = (P(("dp", "cent"), None), P(("dp", "cent")), P(("dp", "cent"), None), P())
    out_specs = (P(("dp", "cent")), P(("dp", "cent")), P(None, ("dp", "cent")))
    return jax.shard_map(local, mesh=mesh, in_specs=in_specs, out_specs=out_specs, check_vma=False)
```

```python
import functools
import math

import jax
import jax.numpy as jnp
from jax import lax
from jax.experimental import pallas as pl
from jax.experimental.pallas import tpu as pltpu
from jax.sharding import PartitionSpec as P

F32 = jnp.float32
BF16 = jnp.bfloat16
LANES = 128
SUB = 8


def round_up(value, unit):
    return -(-value // unit) * unit


def each(low, high, body):
    if high - low <= 8:
        for step in range(low, high):
            body(step)
    else:
        lax.fori_loop(low, high, lambda step, carry: (body(step), carry)[1], 0)


def iota(shape, dim):
    return lax.broadcasted_iota(jnp.int32, shape, dim)


def mm(left, right):
    return lax.dot_general(left, right, (((1,), (0,)), ((), ())), preferred_element_type=F32)


def mm_t(left, right):
    return lax.dot_general(left, right, (((1,), (1,)), ((), ())), preferred_element_type=F32)


def one_hot(condition):
    return jnp.where(condition, 1.0, 0.0).astype(BF16)


def split3(value):
    high = value.astype(BF16)
    rest = value - high.astype(F32)
    mid = rest.astype(BF16)
    low = (rest - mid.astype(F32)).astype(BF16)
    return high, mid, low


def kernel(
    dims,
    docs_hbm,
    assigned_hbm,
    cent_hbm,
    table_hbm,
    out_ref,
    docs_ref,
    assigned_ref,
    table_ref,
    all_buf,
    send_buf,
    chunk_buf,
    code_send,
    code_recv,
    fwd_buf,
    tbl_send,
    tbl_recv,
    res_send,
    res_recv,
    res_rows,
    tag_row,
    tag_mat,
    inv_row,
    inv_mat,
    sim_row,
    best_row,
    best_mat,
    cent_mat,
    gram_acc,
    stats_ref,
    in_sem,
    a_send,
    a_recv,
    m_send,
    m_recv,
    f_send,
    f_recv,
    t_send,
    t_recv,
    r_send,
    r_recv,
):
    R, C, K, Q, PIECES = dims
    O = R * C
    CK = C * K
    L, D = docs_ref.shape
    S = cent_hbm.shape[0]
    T = table_ref.shape[0]
    W = D // PIECES
    QP = code_send.shape[2]
    small = R <= 8
    row_me = lax.axis_index("dp")
    col_me = lax.axis_index("cent")
    own = row_me * C + col_me

    bits = []
    while 2 ** len(bits) < R:
        bits.append(lax.rem(lax.div(row_me, 2 ** len(bits)), 2))
    col_of = [col_me] + [lax.rem(col_me + d, C) for d in range(1, C)]

    def row_of(t):
        total = 0
        for i, bit in enumerate(bits):
            if isinstance(t, int):
                total = total + (1 - bit if (t >> i) & 1 else bit) * 2**i
            else:
                total = total + lax.rem(bit + lax.div(t, 2**i), 2) * 2**i
        return total

    def all_peers(body):
        def at_row(t):
            r = row_of(t)
            for d in range(C):
                body(t, r, d)

        each(1, R, at_row)
        for d in range(1, C):
            body(0, row_me, d)

    def where_is(r, c):
        return {"dp": r, "cent": c}

    def remote(src, dst, send, recv, r, c):
        return pltpu.make_async_remote_copy(
            src_ref=src,
            dst_ref=dst,
            send_sem=send,
            recv_sem=recv,
            device_id=where_is(r, c),
            device_id_type=pl.DeviceIdType.MESH,
        )

    barrier = pltpu.get_barrier_semaphore()

    def greet(t, r, d):
        pl.semaphore_signal(
            barrier, inc=1, device_id=where_is(r, col_of[d]), device_id_type=pl.DeviceIdType.MESH
        )

    all_peers(greet)

    cent_rows = all_buf.at[pl.ds(0, S), :]
    loads = [
        pltpu.make_async_copy(assigned_hbm, assigned_ref, in_sem.at[0]),
        pltpu.make_async_copy(table_hbm, table_ref, in_sem.at[1]),
        pltpu.make_async_copy(docs_hbm, docs_ref, in_sem.at[2]),
        pltpu.make_async_copy(cent_hbm, cent_rows, in_sem.at[3]),
    ]
    for load in loads:
        load.start()
    loads[0].wait()
    loads[1].wait()

    assigned = assigned_ref[...]
    high = lax.shift_right_logical(assigned, 7)
    low = jnp.bitwise_and(assigned, 127)
    table = table_ref[...]
    pick = one_hot(iota((T, L), 0) == high)
    looked = jnp.zeros((LANES, L), F32)
    shift = 0
    while 2**shift < O * S:
        digit = jnp.bitwise_and(lax.shift_right_logical(table, shift), 255)
        looked = looked + float(2**shift) * lax.dot_general(
            digit.astype(F32).astype(BF16), pick, (((0,), (0,)), ((), ())), preferred_element_type=F32
        )
        shift += 8
    slot = jnp.sum(jnp.where(iota((LANES, L), 0) == low, looked, 0.0), axis=0, keepdims=True)
    owner = jnp.floor((slot + 0.5) * (1.0 / S))
    row = jnp.floor((owner + 0.5) * (1.0 / C))
    owner_i = owner.astype(jnp.int32)
    row_i = row.astype(jnp.int32)
    cent_i = owner_i - row_i * C
    is_owner = jnp.where(iota((O, L), 0) == owner_i, 1.0, 0.0)
    is_row = jnp.where(iota((R, L), 0) == row_i, 1.0, 0.0)
    earlier = one_hot(iota((L, L), 0) < iota((L, L), 1))
    ranks = mm(jnp.concatenate([is_owner, is_row], axis=0).astype(BF16), earlier)
    rank_owner = jnp.sum(ranks[:O] * is_owner, axis=0, keepdims=True)
    rank_row = jnp.sum(ranks[O:] * is_row, axis=0, keepdims=True)
    position = jnp.bitwise_xor(row_i, row_me) * Q + rank_row.astype(jnp.int32)
    rank_i = rank_owner.astype(jnp.int32)

    ahead = cent_i - col_me
    ahead = jnp.where(ahead < 0, ahead + C, ahead)
    behind = jnp.where(ahead == 0, 0, C - ahead)
    lane_i = behind * K + rank_i
    code = ((ahead * K + rank_i) + 1).astype(F32).astype(BF16)
    code8 = jnp.broadcast_to(code, (SUB, L))
    is_lane = one_hot(iota((LANES, L), 0) == lane_i)

    tag = slot - owner * S + 1.0
    tag_hi = jnp.floor(tag * (1.0 / 128.0))
    tag_lo = tag - tag_hi * 128.0
    tags = mm_t(jnp.concatenate([is_owner * tag_hi, is_owner * tag_lo], axis=0).astype(BF16), is_lane)
    tags = 128.0 * tags[:O] + tags[O:]
    for o in range(O):
        tbl_send[o] = tags[o : o + 1, :]

    def mark(t):
        line = mm_t(code8, one_hot(iota((QP, L), 0) + t * Q == jnp.where(position < (t + 1) * Q, position, -1)))
        code_send[t] = line[0:1, :]

    each(0, R, mark)

    def row_copy(t, p):
        at = pl.ds(p * W, W)
        return remote(
            send_buf.at[t, :, at], chunk_buf.at[t, :, at], a_send.at[0], a_recv.at[t, p], row_of(t), col_me
        )

    def code_copy(t):
        return remote(code_send.at[t], code_recv.at[t], m_send.at[0], m_recv.at[0], row_of(t), col_me)

    def tbl_copy(t, r, d):
        return remote(
            tbl_send.at[r * C + col_of[d]],
            tbl_recv.at[t * C + (C - d) % C],
            t_send.at[0],
            t_recv.at[0],
            r,
            col_of[d],
        )

    def whole(ref, send, recv):
        return remote(ref, ref, send.at[0], recv.at[0], row_of(1), col_me)

    tbl_all = whole(tbl_recv.at[pl.ds(1, O - 1)], t_send, t_recv)
    code_all = whole(code_recv.at[pl.ds(1, R - 1)], m_send, m_recv)

    def start_rows(t):
        for p in range(PIECES):
            row_copy(t, p).start()

    def choose(ts):
        wanted = [one_hot(iota((Q, L), 0) + t * Q == position) for t in ts]
        found = mm(jnp.concatenate(wanted, axis=0), docs_ref[...]).astype(BF16)
        for i, t in enumerate(ts):
            send_buf[t] = found[i * Q : (i + 1) * Q]

    def first_sends():
        pl.semaphore_wait(barrier, O - 1)
        each(1, R, lambda t: code_copy(t).start())
        all_peers(lambda t, r, d: tbl_copy(t, r, d).start())

    loads[2].wait()
    if R == 8:
        inner = lax.rem(bits[-1] + bits[-2], 2) == 1
        far = R // 2
        choose([far, 2])
        first_sends()

        @pl.when(inner)
        def _():
            start_rows(far)

        start_rows(2)
        choose([3, 1])
        start_rows(3)

        @pl.when(jnp.logical_not(inner))
        def _():
            start_rows(far)

        start_rows(1)
        choose([5, 6])
        start_rows(5)
        start_rows(6)
        choose([7, 0])
        start_rows(7)
    else:
        first_sends()
        group = max(1, R // 2)
        for first in range(0, R, group):
            wanted = one_hot(iota((group * Q, L), 0) + first * Q == position)
            send_buf[first : first + group] = (
                mm(wanted, docs_ref[...]).astype(BF16).reshape(group, Q, D)
            )
            each(max(first, 1), first + group, start_rows)
    tbl_recv[0] = tbl_send[own]

    def rows_at(t, block=0, count=None):
        return pl.ds(S + t * CK + block * K, CK if count is None else count)

    def fwd_copy(t, d, p):
        at = pl.ds(p * W, W)
        return remote(
            fwd_buf.at[t, d - 1, :, at],
            all_buf.at[rows_at(t, C - d, K), at],
            f_send.at[0],
            f_recv.at[t, p],
            row_me,
            col_of[d],
        )

    def fwd_arrival(t, p):
        ref = all_buf.at[rows_at(t, 1, CK - K), pl.ds(p * W, W)]
        return remote(ref, ref, f_send.at[0], f_recv.at[t, p], row_me, col_of[1])

    def relay(t, p, mine=False):
        if not mine:
            row_copy(t, p).wait_recv()
        at = pl.ds(p * W, W)
        line = (code_send if mine else code_recv)[t][:, :Q].astype(jnp.int32)
        wanted = one_hot(iota((CK, Q), 0) + 1 == line)
        found = mm(wanted, (send_buf if mine else chunk_buf)[t, :, at]).astype(BF16)
        fwd_buf[t, :, :, at] = found[K:].reshape(C - 1, K, W)
        for d in range(1, C):
            fwd_copy(t, d, p).start()
        all_buf[rows_at(t, 0, K), at] = found[:K]

    for p in range(PIECES):
        relay(0, p, True)

    loads[3].wait()
    norm = jnp.zeros((S, LANES), F32)
    for part in range(0, D, LANES):
        block = all_buf[0:S, part : part + LANES].astype(F32)
        norm = norm + block * block
    cent_mat[...] = jnp.broadcast_to(
        lax.rsqrt(jnp.sum(norm, axis=1, keepdims=True) + 1.0), cent_mat.shape
    )

    tbl_all.wait_recv()
    code_all.wait_recv()

    eye = iota((CK, CK), 0) == iota((CK, CK), 1)

    def spread(t):
        line = tbl_recv[t * C]
        for c in range(1, C):
            line = line + tbl_recv[t * C + c]
        line = line[:, :CK]
        tag_row[t] = line
        tag_mat[t] = jnp.broadcast_to(
            jnp.sum(jnp.where(eye, line, 0.0), axis=1, keepdims=True), (CK, CK)
        )
        best_mat[t] = jnp.zeros((CK, CK), F32)

    each(0, R, spread)
    stats_ref[...] = jnp.zeros(stats_ref.shape, F32)

    def member_of(t):
        return (iota((S, CK), 0) + 1).astype(F32) == tag_row[t]

    def self_block(t, gram):
        diag = jnp.where(eye, gram, 0.0)
        row_scale = lax.rsqrt(jnp.sum(diag, axis=0, keepdims=True) + 1.0)
        col_scale = lax.rsqrt(jnp.sum(diag, axis=1, keepdims=True) + 1.0)
        inv_row[t] = row_scale
        inv_mat[t] = jnp.broadcast_to(col_scale, (CK, CK))
        line = jnp.where(tag_row[t] > 0.0, tag_row[t], -1.0)
        same = (tag_mat[t] == line) & jnp.logical_not(eye)
        best = jnp.max(jnp.where(same, gram * col_scale, 0.0), axis=0, keepdims=True)
        return row_scale, line, best

    def other_block(u, gram, row_scale, line, best):
        same = tag_mat[u] == line
        best_mat[u] = jnp.maximum(best_mat[u], jnp.where(same, gram * row_scale, 0.0))
        return jnp.maximum(
            best, jnp.max(jnp.where(same, gram * inv_mat[u], 0.0), axis=0, keepdims=True)
        )

    def cross_block(t, cross, row_scale):
        member = member_of(t)
        similarity = row_scale * jnp.sum(
            jnp.where(member, cross * cent_mat[...], 0.0), axis=0, keepdims=True
        )
        sim_row[t] = similarity
        lines = [jnp.ones((1, CK), BF16), *split3(similarity), *split3(similarity * similarity)]
        lines = jnp.concatenate(
            [line.astype(F32) for line in lines] + [jnp.zeros((1, CK), F32)], axis=0
        )
        stats_ref[...] += mm_t(lines.astype(BF16), one_hot(member))

    def settle(t, read):
        row_scale, line, best = self_block(t, read(S + t * CK, CK))
        for u in range(t):
            best = other_block(u, read(S + u * CK, CK), row_scale, line, best)
        best_row[t] = best
        cross_block(t, read(0, S), row_scale)

    def arrivals(t, p):
        fwd_arrival(t, p).wait_recv()

    def absorb_piece(t, p):
        arrivals(t, p)
        at = pl.ds(p * W, W)
        rows = S + (t + 1) * CK
        part = mm_t(all_buf[0:rows, at], all_buf[rows_at(t), at])
        gram_acc[0:rows] = part if p == 0 else gram_acc[0:rows] + part
        if p == PIECES - 1:
            settle(t, lambda start, count: gram_acc[start : start + count])

    def absorb(t):
        for p in range(PIECES):
            absorb_piece(t, p)

    def absorb_any(t):
        for p in range(PIECES):
            arrivals(t, p)
        mine = all_buf[rows_at(t), :]
        row_scale, line, best = self_block(t, mm_t(mine, mine))

        def pair(u, best):
            return other_block(u, mm_t(all_buf[rows_at(u), :], mine), row_scale, line, best)

        best_row[t] = lax.fori_loop(0, t, pair, best)
        cross_block(t, mm_t(all_buf[0:S, :], mine), row_scale)

    def relay_all(t):
        for p in range(PIECES):
            relay(t, p)

    if small:
        done = 0
        for t in range(1, R - 2):
            relay_all(t)
            while done < (t + 1 if t == R - 3 else t):
                absorb(done)
                done += 1
        steps = [(t, p) for t in (R - 2, R - 1) for p in range(PIECES)]
        lag = 2
        for i in range(len(steps) + lag):
            if i < len(steps):
                relay(*steps[i])
            if i >= lag:
                absorb_piece(*steps[i - lag])
    else:

        def advance(t, carry):
            relay_all(t)
            absorb_any(t - 1)
            return carry

        lax.fori_loop(1, R, advance, 0)
        absorb_any(R - 1)

    stats = stats_ref[...]
    count = stats[0:1]
    total = stats[1:2] + stats[2:3] + stats[3:4]
    square = stats[4:5] + stats[5:6] + stats[6:7]
    floor = jnp.maximum(count, 1.0)
    mean = total / floor
    variance = jnp.maximum(square / floor - mean * mean, 0.0)
    spread_inv = 1.0 / jnp.sqrt(variance + 1.0 / D)
    wanted = [line.astype(F32) for line in (*split3(mean), *split3(spread_inv))]
    wanted = jnp.concatenate(wanted + [jnp.zeros((2, S), F32)], axis=0).astype(BF16)

    def res_copy(t, r, d):
        return remote(
            res_send.at[t], res_recv.at[t * C + (C - d) % C], r_send.at[0], r_recv.at[0], r, col_of[d]
        )

    res_all = whole(res_recv.at[pl.ds(1, O - 1)], r_send, r_recv)

    def finish(t, found):
        centre = found[0:1] + found[1:2] + found[2:3]
        width = found[3:4] + found[4:5] + found[5:6]
        proto = (centre - sim_row[t]) * width
        column = jnp.max(best_mat[t], axis=1, keepdims=True)
        flat = jnp.max(jnp.where(eye, column, 0.0), axis=0, keepdims=True)
        redundant = jnp.maximum(flat, best_row[t]) * inv_row[t] * math.sqrt(D)
        res_send[t, 0:1, :CK] = proto
        res_send[t, 1:2, :CK] = redundant

    if CK < LANES:
        res_send[...] = jnp.zeros(res_send.shape, F32)

    def deliver(t):
        r = row_of(t)
        for d in (2, 3, 1, 0) if C == 4 else range(C):
            if not (isinstance(t, int) and t == 0 and d == 0):
                res_copy(t, r, d).start()

    if small:
        members = jnp.concatenate([one_hot(member_of(t)) for t in range(R)], axis=1)
        found = mm(wanted, members)
        for t in range(R):
            finish(t, found[:, t * CK : (t + 1) * CK])
        for t in [5, 4, 7, 6, 3, 2, 1, 0] if R == 8 else range(R):
            deliver(t)
    else:

        def finish_any(t):
            finish(t, mm(wanted, one_hot(member_of(t))))

        each(0, R, finish_any)
        each(1, R, deliver)
        deliver(0)
    res_recv[0] = res_send[0]
    out_ref[2:3, :S] = count
    out_ref[3:4, :S] = total
    out_ref[4:5, :S] = square

    remote(
        send_buf.at[pl.ds(1, R - 1)], send_buf.at[pl.ds(1, R - 1)], a_send.at[0], a_recv.at[0, 0], row_of(1), col_me
    ).wait_send()
    code_all.wait_send()
    tbl_all.wait_send()
    remote(fwd_buf, fwd_buf, f_send.at[0], f_recv.at[0, 0], row_me, col_of[1]).wait_send()
    res_all.wait_send()
    res_all.wait_recv()

    for o in range(O):
        pair = res_recv[o]
        res_rows[o : o + 1, :] = pair[0:1]
        res_rows[O + o : O + o + 1, :] = pair[1:2]
    parts = jnp.concatenate([line.astype(F32) for line in split3(res_rows[...])], axis=0)
    found = mm(parts.astype(BF16), is_lane)
    found = found[: 2 * O] + found[2 * O : 4 * O] + found[4 * O :]
    mask = iota((O, L), 0) == jnp.bitwise_xor(row_i, row_me) * C + ahead
    out_ref[0:1, :L] = jnp.sum(jnp.where(mask, found[:O], 0.0), axis=0, keepdims=True)
    out_ref[1:2, :L] = jnp.sum(jnp.where(mask, found[O:], 0.0), axis=0, keepdims=True)


def local(documents, assigned, centroids, owner_slot):
    L, D = documents.shape
    S = centroids.shape[0]
    R = lax.axis_size("dp")
    C = lax.axis_size("cent")
    O = R * C
    pair_cap = 2 * L // O
    row_cap = 5 * C * pair_cap // 8
    K = round_up(pair_cap, 16)
    Q = round_up(row_cap, 16)
    CK = C * K
    QP = round_up(Q, LANES)
    pieces = 4 if R <= 8 else 1
    T = owner_slot.shape[0] // LANES
    hbm = pl.BlockSpec(memory_space=pl.ANY)
    dma = pltpu.SemaphoreType.DMA
    packed = pl.pallas_call(
        functools.partial(kernel, (R, C, K, Q, pieces)),
        name="cluster_exchange",
        out_shape=jax.ShapeDtypeStruct((SUB, max(L, S)), F32),
        in_specs=[hbm] * 4,
        out_specs=pl.BlockSpec(memory_space=pltpu.VMEM),
        scratch_shapes=[
            pltpu.VMEM((L, D), BF16),
            pltpu.VMEM((1, L), jnp.int32),
            pltpu.VMEM((T, LANES), jnp.int32),
            pltpu.VMEM((S + R * CK, D), BF16),
            pltpu.VMEM((R, Q, D), BF16),
            pltpu.VMEM((R, Q, D), BF16),
            pltpu.VMEM((R, 1, QP), F32),
            pltpu.VMEM((R, 1, QP), F32),
            pltpu.VMEM((R, C - 1, K, D), BF16),
            pltpu.VMEM((O, 1, LANES), F32),
            pltpu.VMEM((O, 1, LANES), F32),
            pltpu.VMEM((R, 2, LANES), F32),
            pltpu.VMEM((O, 2, LANES), F32),
            pltpu.VMEM((2 * O, LANES), F32),
            pltpu.VMEM((R, 1, CK), F32),
            pltpu.VMEM((R, CK, CK), F32),
            pltpu.VMEM((R, 1, CK), F32),
            pltpu.VMEM((R, CK, CK), F32),
            pltpu.VMEM((R, 1, CK), F32),
            pltpu.VMEM((R, 1, CK), F32),
            pltpu.VMEM((R, CK, CK), F32),
            pltpu.VMEM((S, CK), F32),
            pltpu.VMEM((S + R * CK if R <= 8 else SUB, CK), F32),
            pltpu.VMEM((SUB, S), F32),
            dma((4,)),
            dma((1,)),
            dma((R, pieces)),
            dma((1,)),
            dma((1,)),
            dma((1,)),
            dma((R, pieces)),
            dma((1,)),
            dma((1,)),
            dma((1,)),
            dma((1,)),
        ],
        compiler_params=pltpu.CompilerParams(
            collective_id=0, has_side_effects=True, vmem_limit_bytes=62 * 1024 * 1024
        ),
    )(
        documents,
        assigned.reshape(1, L),
        centroids,
        owner_slot.reshape(-1, LANES),
    )
    return packed[0, :L], packed[1, :L], packed[2:5, :S]


def solution(mesh):
    in_specs = (P(("dp", "cent"), None), P(("dp", "cent")), P(("dp", "cent"), None), P())
    out_specs = (P(("dp", "cent")), P(("dp", "cent")), P(None, ("dp", "cent")))
    return jax.shard_map(local, mesh=mesh, in_specs=in_specs, out_specs=out_specs, check_vma=False)
```

```python
import functools
import math

import jax
import jax.numpy as jnp
from jax import lax
from jax.experimental import pallas as pl
from jax.experimental.pallas import tpu as pltpu
from jax.sharding import PartitionSpec as P

F32 = jnp.float32
BF16 = jnp.bfloat16
LANES = 128
SUB = 8


def round_up(value, unit):
    return -(-value // unit) * unit


def each(low, high, body):
    if high - low <= 8:
        for step in range(low, high):
            body(step)
    else:
        lax.fori_loop(low, high, lambda step, carry: (body(step), carry)[1], 0)


def iota(shape, dim):
    return lax.broadcasted_iota(jnp.int32, shape, dim)


def mm(left, right):
    return lax.dot_general(left, right, (((1,), (0,)), ((), ())), preferred_element_type=F32)


def mm_t(left, right):
    return lax.dot_general(left, right, (((1,), (1,)), ((), ())), preferred_element_type=F32)


def one_hot(condition):
    return jnp.where(condition, 1.0, 0.0).astype(BF16)


def split3(value):
    high = value.astype(BF16)
    rest = value - high.astype(F32)
    mid = rest.astype(BF16)
    low = (rest - mid.astype(F32)).astype(BF16)
    return high, mid, low


def kernel(
    dims,
    docs_hbm,
    assigned_hbm,
    cent_hbm,
    table_hbm,
    out_ref,
    docs_ref,
    assigned_ref,
    table_ref,
    all_buf,
    send_buf,
    chunk_buf,
    code_send,
    code_recv,
    fwd_buf,
    tag_send,
    tag_recv,
    res_send,
    res_recv,
    res_rows,
    tag_row,
    tag_mat,
    inv_row,
    inv_mat,
    sim_row,
    best_row,
    best_mat,
    cent_mat,
    gram_acc,
    stats_ref,
    in_sem,
    a_send,
    a_recv,
    m_send,
    m_recv,
    f_send,
    f_recv,
    t_send,
    t_recv,
    r_send,
    r_recv,
):
    R, C, K, Q, cuts = dims
    O = R * C
    CK = C * K
    L, D = docs_ref.shape
    S = cent_hbm.shape[0]
    T = table_ref.shape[0]
    QP = code_send.shape[2]
    small = R <= 8
    row_me = lax.axis_index("dp")
    col_me = lax.axis_index("cent")
    own = row_me * C + col_me

    bits = []
    while 2 ** len(bits) < R:
        bits.append(lax.rem(lax.div(row_me, 2 ** len(bits)), 2))
    col_of = [col_me] + [lax.rem(col_me + d, C) for d in range(1, C)]

    swap = {3: 4, 4: 3} if R == 8 else {}

    def row_of(t):
        total = 0
        if isinstance(t, int):
            t = swap.get(t, t)
        for i, bit in enumerate(bits):
            if isinstance(t, int):
                total = total + (1 - bit if (t >> i) & 1 else bit) * 2**i
            else:
                total = total + lax.rem(bit + lax.div(t, 2**i), 2) * 2**i
        return total

    def all_peers(body):
        def at_row(t):
            r = row_of(t)
            for d in range(C):
                body(t, r, d)

        each(1, R, at_row)
        for d in range(1, C):
            body(0, row_me, d)

    def where_is(r, c):
        return {"dp": r, "cent": c}

    def remote(src, dst, send, recv, r, c):
        return pltpu.make_async_remote_copy(
            src_ref=src,
            dst_ref=dst,
            send_sem=send,
            recv_sem=recv,
            device_id=where_is(r, c),
            device_id_type=pl.DeviceIdType.MESH,
        )

    barrier = pltpu.get_barrier_semaphore()

    def greet(r, c):
        pl.semaphore_signal(
            barrier, inc=1, device_id=where_is(r, c), device_id_type=pl.DeviceIdType.MESH
        )

    each(1, R, lambda t: greet(row_of(t), col_me))
    for d in range(1, C):
        greet(row_me, col_of[d])

    cent_rows = all_buf.at[pl.ds(0, S), :]
    loads = [
        pltpu.make_async_copy(assigned_hbm, assigned_ref, in_sem.at[0]),
        pltpu.make_async_copy(table_hbm, table_ref, in_sem.at[1]),
        pltpu.make_async_copy(docs_hbm, docs_ref, in_sem.at[2]),
        pltpu.make_async_copy(cent_hbm, cent_rows, in_sem.at[3]),
    ]
    for load in loads:
        load.start()
    loads[0].wait()
    loads[1].wait()

    assigned = assigned_ref[...]
    high = lax.shift_right_logical(assigned, 7)
    low = jnp.bitwise_and(assigned, 127)
    table = table_ref[...]
    pick = one_hot(iota((T, L), 0) == high)
    looked = jnp.zeros((LANES, L), F32)
    shift = 0
    while 2**shift < O * S:
        digit = jnp.bitwise_and(lax.shift_right_logical(table, shift), 255)
        looked = looked + float(2**shift) * lax.dot_general(
            digit.astype(F32).astype(BF16), pick, (((0,), (0,)), ((), ())), preferred_element_type=F32
        )
        shift += 8
    slot = jnp.sum(jnp.where(iota((LANES, L), 0) == low, looked, 0.0), axis=0, keepdims=True)
    owner = jnp.floor((slot + 0.5) * (1.0 / S))
    row = jnp.floor((owner + 0.5) * (1.0 / C))
    owner_i = owner.astype(jnp.int32)
    row_i = row.astype(jnp.int32)
    cent_i = owner_i - row_i * C
    is_owner = jnp.where(iota((O, L), 0) == owner_i, 1.0, 0.0)
    is_row = jnp.where(iota((R, L), 0) == row_i, 1.0, 0.0)
    earlier = one_hot(iota((L, L), 0) < iota((L, L), 1))
    ranks = mm(jnp.concatenate([is_owner, is_row], axis=0).astype(BF16), earlier)
    rank_owner = jnp.sum(ranks[:O] * is_owner, axis=0, keepdims=True)
    rank_row = jnp.sum(ranks[O:] * is_row, axis=0, keepdims=True)
    block_i = jnp.bitwise_xor(row_i, row_me)
    if swap:
        block_i = jnp.where((block_i == 3) | (block_i == 4), 7 - block_i, block_i)
    position = block_i * Q + rank_row.astype(jnp.int32)
    rank_i = rank_owner.astype(jnp.int32)

    ahead = cent_i - col_me
    ahead = jnp.where(ahead < 0, ahead + C, ahead)
    behind = jnp.where(ahead == 0, 0, C - ahead)
    lane_i = behind * K + rank_i
    is_lane = one_hot(iota((LANES, L), 0) == lane_i)

    tag = slot - owner * S + 1.0
    tag_hi = jnp.floor(tag * (1.0 / 128.0))
    lines = jnp.concatenate(
        [(ahead * K + rank_i + 1).astype(F32), tag_hi, tag - tag_hi * 128.0, jnp.zeros((SUB - 3, L), F32)],
        axis=0,
    ).astype(BF16)

    def mark(t):
        here = jnp.where(position < (t + 1) * Q, position, -1)
        line = mm_t(lines, one_hot(iota((QP, L), 0) + t * Q == here))
        code_send[t, 0:1, :] = line[0:1]
        code_send[t, 1:2, :] = 128.0 * line[1:2] + line[2:3]

    each(0, R, mark)

    def cut(t, p):
        width = cuts[t][p] if small else D
        return pl.ds(sum(cuts[t][:p]) if small else 0, width), width

    def sem(t, p):
        return sum(len(c) for c in cuts[:t]) + p if small else t

    def pieces(t):
        return range(len(cuts[t])) if small else range(1)

    def row_copy(t, p):
        at = cut(t, p)[0]
        return remote(
            send_buf.at[t, :, at], chunk_buf.at[t, :, at], a_send.at[0], a_recv.at[sem(t, p)], row_of(t), col_me
        )

    def code_copy(t):
        return remote(code_send.at[t], code_recv.at[t], m_send.at[0], m_recv.at[0], row_of(t), col_me)

    def whole(ref, send, recv):
        return remote(ref, ref, send.at[0], recv.at[0], row_of(1), col_me)

    code_all = whole(code_recv.at[pl.ds(1, R - 1)], m_send, m_recv)

    def start_rows(t):
        for p in pieces(t):
            row_copy(t, p).start()

    def choose(ts):
        wanted = [one_hot(iota((Q, L), 0) + t * Q == position) for t in ts]
        found = mm(jnp.concatenate(wanted, axis=0), docs_ref[...]).astype(BF16)
        for i, t in enumerate(ts):
            send_buf[t] = found[i * Q : (i + 1) * Q]

    def first_sends():
        pl.semaphore_wait(barrier, R + C - 2)
        each(1, R, lambda t: code_copy(t).start())

    loads[2].wait()
    if R == 8:
        inner = lax.rem(bits[-1] + bits[-2], 2) == 1
        choose([3, 1])
        first_sends()

        @pl.when(inner)
        def _():
            start_rows(3)

        start_rows(1)
        choose([2, 4])
        start_rows(2)
        start_rows(4)

        @pl.when(jnp.logical_not(inner))
        def _():
            start_rows(3)

        choose([5, 6])
        start_rows(5)
        start_rows(6)
        choose([7, 0])
        start_rows(7)
    else:
        first_sends()
        group = max(1, R // 2)
        for first in range(0, R, group):
            wanted = one_hot(iota((group * Q, L), 0) + first * Q == position)
            send_buf[first : first + group] = (
                mm(wanted, docs_ref[...]).astype(BF16).reshape(group, Q, D)
            )
            each(max(first, 1), first + group, start_rows)

    def rows_at(t, block=0, count=None):
        return pl.ds(S + t * CK + block * K, CK if count is None else count)

    def fwd_copy(t, d, p):
        at = cut(t, p)[0]
        return remote(
            fwd_buf.at[t, d - 1, :, at],
            all_buf.at[rows_at(t, C - d, K), at],
            f_send.at[0],
            f_recv.at[sem(t, p)],
            row_me,
            col_of[d],
        )

    def fwd_arrival(t, p):
        ref = all_buf.at[rows_at(t, 1, CK - K), cut(t, p)[0]]
        return remote(ref, ref, f_send.at[0], f_recv.at[sem(t, p)], row_me, col_of[1])

    def tag_copy(t, d):
        return remote(
            tag_send.at[t], tag_recv.at[t, C - d], t_send.at[0], t_recv.at[t], row_me, col_of[d]
        )

    def tag_arrival(t):
        ref = tag_recv.at[t, pl.ds(1, C - 1)]
        return remote(ref, ref, t_send.at[0], t_recv.at[t], row_me, col_of[1])

    block = iota((CK, Q), 0) // K
    turned = jnp.where(block == 0, 0, C - block) * K + iota((CK, Q), 0) - block * K + 1

    def relay(t, p, mine=False):
        if not mine:
            row_copy(t, p).wait_recv()
        at, width = cut(t, p)
        lines = (code_send if mine else code_recv)[t][:, :Q]
        line = lines[0:1].astype(jnp.int32)
        wanted = one_hot(iota((CK, Q), 0) + 1 == line)
        if p == 0:
            high = jnp.floor(lines[1:2] * (1.0 / 128.0))
            digits = [high, lines[1:2] - high * 128.0, jnp.zeros((SUB - 2, Q), F32)]
            digits = mm_t(jnp.concatenate(digits, axis=0).astype(BF16), one_hot(turned == line))
            tag_send[t, 0:1, :CK] = 128.0 * digits[0:1] + digits[1:2]
            for d in range(1, C):
                tag_copy(t, d).start()
        found = mm(wanted, (send_buf if mine else chunk_buf)[t, :, at]).astype(BF16)
        fwd_buf[t, :, :, at] = found[K:].reshape(C - 1, K, width)
        for d in range(1, C):
            fwd_copy(t, d, p).start()
        all_buf[rows_at(t, 0, K), at] = found[:K]

    if CK < LANES:
        tag_send[...] = jnp.zeros(tag_send.shape, F32)
    for p in pieces(0):
        relay(0, p, True)
    code_all.wait_recv()

    loads[3].wait()
    norm = jnp.zeros((S, LANES), F32)
    for part in range(0, D, LANES):
        block = all_buf[0:S, part : part + LANES].astype(F32)
        norm = norm + block * block
    cent_mat[...] = jnp.broadcast_to(
        lax.rsqrt(jnp.sum(norm, axis=1, keepdims=True) + 1.0), cent_mat.shape
    )


    eye = iota((CK, CK), 0) == iota((CK, CK), 1)

    def spread(t):
        tag_arrival(t).wait_recv()
        line = tag_send[t][:, :CK]
        for c in range(1, C):
            line = jnp.where(iota((1, CK), 1) // K == c, tag_recv[t, c][:, :CK], line)
        tag_row[t] = line
        tag_mat[t] = jnp.broadcast_to(
            jnp.sum(jnp.where(eye, line, 0.0), axis=1, keepdims=True), (CK, CK)
        )
        best_mat[t] = jnp.zeros((CK, CK), F32)

    stats_ref[...] = jnp.zeros(stats_ref.shape, F32)

    def member_of(t):
        return (iota((S, CK), 0) + 1).astype(F32) == tag_row[t]

    def self_block(t, gram):
        diag = jnp.where(eye, gram, 0.0)
        row_scale = lax.rsqrt(jnp.sum(diag, axis=0, keepdims=True) + 1.0)
        col_scale = lax.rsqrt(jnp.sum(diag, axis=1, keepdims=True) + 1.0)
        inv_row[t] = row_scale
        inv_mat[t] = jnp.broadcast_to(col_scale, (CK, CK))
        line = jnp.where(tag_row[t] > 0.0, tag_row[t], -1.0)
        same = (tag_mat[t] == line) & jnp.logical_not(eye)
        best = jnp.max(jnp.where(same, gram * col_scale, 0.0), axis=0, keepdims=True)
        return row_scale, line, best

    def other_block(u, gram, row_scale, line, best):
        same = tag_mat[u] == line
        best_mat[u] = jnp.maximum(best_mat[u], jnp.where(same, gram * row_scale, 0.0))
        return jnp.maximum(
            best, jnp.max(jnp.where(same, gram * inv_mat[u], 0.0), axis=0, keepdims=True)
        )

    def cross_block(t, cross, row_scale):
        member = member_of(t)
        similarity = row_scale * jnp.sum(
            jnp.where(member, cross * cent_mat[...], 0.0), axis=0, keepdims=True
        )
        sim_row[t] = similarity
        lines = [jnp.ones((1, CK), BF16), *split3(similarity), *split3(similarity * similarity)]
        lines = jnp.concatenate(
            [line.astype(F32) for line in lines] + [jnp.zeros((1, CK), F32)], axis=0
        )
        stats_ref[...] += mm_t(lines.astype(BF16), one_hot(member))

    def settle(t, read):
        row_scale, line, best = self_block(t, read(S + t * CK, CK))
        for u in range(t):
            best = other_block(u, read(S + u * CK, CK), row_scale, line, best)
        best_row[t] = best
        cross_block(t, read(0, S), row_scale)

    def arrivals(t, p):
        fwd_arrival(t, p).wait_recv()

    def absorb_piece(t, p):
        if p == 0:
            spread(t)
        arrivals(t, p)
        at = cut(t, p)[0]
        rows = S + (t + 1) * CK
        part = mm_t(all_buf[0:rows, at], all_buf[rows_at(t), at])
        gram_acc[0:rows] = part if p == 0 else gram_acc[0:rows] + part
        if p == len(cuts[t]) - 1:
            settle(t, lambda start, count: gram_acc[start : start + count])

    def absorb(t):
        for p in pieces(t):
            absorb_piece(t, p)

    def absorb_any(t):
        spread(t)
        arrivals(t, 0)
        mine = all_buf[rows_at(t), :]
        row_scale, line, best = self_block(t, mm_t(mine, mine))

        def pair(u, best):
            return other_block(u, mm_t(all_buf[rows_at(u), :], mine), row_scale, line, best)

        best_row[t] = lax.fori_loop(0, t, pair, best)
        cross_block(t, mm_t(all_buf[0:S, :], mine), row_scale)

    def relay_all(*ts):
        for p in pieces(ts[0]):
            for t in ts:
                relay(t, p)

    if R == 8:
        relay_all(1)
        absorb(0)
        relay_all(2, 3)
        absorb(1)
        relay(4, 0)
        relay(5, 0)
        absorb(2)
        relay(4, 1)
        relay(5, 1)
        absorb(3)
        absorb(4)
        absorb(5)
        steps = [(t, p) for t in (6, 7) for p in pieces(t)]
        lag = 3
        for i in range(-lag, len(steps)):
            if i + lag < len(steps):
                relay(*steps[i + lag])
            if i >= 0:
                absorb_piece(*steps[i])
    elif small:
        for t in range(1, R):
            relay_all(t)
            absorb(t - 1)
        absorb(R - 1)
    else:

        def advance(t, carry):
            relay_all(t)
            absorb_any(t - 1)
            return carry

        lax.fori_loop(1, R, advance, 0)
        absorb_any(R - 1)

    stats = stats_ref[...]
    count = stats[0:1]
    total = stats[1:2] + stats[2:3] + stats[3:4]
    square = stats[4:5] + stats[5:6] + stats[6:7]
    floor = jnp.maximum(count, 1.0)
    mean = total / floor
    variance = jnp.maximum(square / floor - mean * mean, 0.0)
    spread_inv = 1.0 / jnp.sqrt(variance + 1.0 / D)
    wanted = [line.astype(F32) for line in (*split3(mean), *split3(spread_inv))]
    wanted = jnp.concatenate(wanted + [jnp.zeros((2, S), F32)], axis=0).astype(BF16)

    def res_copy(t, r, d):
        return remote(
            res_send.at[t], res_recv.at[t * C + (C - d) % C], r_send.at[0], r_recv.at[0], r, col_of[d]
        )

    res_all = whole(res_recv.at[pl.ds(1, O - 1)], r_send, r_recv)

    def finish(t, found):
        centre = found[0:1] + found[1:2] + found[2:3]
        width = found[3:4] + found[4:5] + found[5:6]
        proto = (centre - sim_row[t]) * width
        column = jnp.max(best_mat[t], axis=1, keepdims=True)
        flat = jnp.max(jnp.where(eye, column, 0.0), axis=0, keepdims=True)
        redundant = jnp.maximum(flat, best_row[t]) * inv_row[t] * math.sqrt(D)
        res_send[t, 0:1, :CK] = proto
        res_send[t, 1:2, :CK] = redundant

    if CK < LANES:
        res_send[...] = jnp.zeros(res_send.shape, F32)

    def deliver(t):
        r = row_of(t)
        for d in (2, 3, 1, 0) if C == 4 else range(C):
            if not (isinstance(t, int) and t == 0 and d == 0):
                res_copy(t, r, d).start()

    if small:
        members = jnp.concatenate([one_hot(member_of(t)) for t in range(R)], axis=1)
        found = mm(wanted, members)
        for t in range(R):
            finish(t, found[:, t * CK : (t + 1) * CK])
        for t in [5, 3, 7, 6, 4, 2, 1, 0] if R == 8 else range(R):
            deliver(t)
    else:

        def finish_any(t):
            finish(t, mm(wanted, one_hot(member_of(t))))

        each(0, R, finish_any)
        each(1, R, deliver)
        deliver(0)
    res_recv[0] = res_send[0]
    out_ref[2:3, :S] = count
    out_ref[3:4, :S] = total
    out_ref[4:5, :S] = square

    remote(
        send_buf.at[pl.ds(1, R - 1)], send_buf.at[pl.ds(1, R - 1)], a_send.at[0], a_recv.at[0], row_of(1), col_me
    ).wait_send()
    code_all.wait_send()
    ref = tag_recv.at[:, pl.ds(1, C - 1)]
    remote(ref, ref, t_send.at[0], t_recv.at[0], row_me, col_of[1]).wait_send()
    remote(fwd_buf, fwd_buf, f_send.at[0], f_recv.at[0], row_me, col_of[1]).wait_send()
    res_all.wait_send()
    res_all.wait_recv()

    for o in range(O):
        pair = res_recv[o]
        res_rows[o : o + 1, :] = pair[0:1]
        res_rows[O + o : O + o + 1, :] = pair[1:2]
    parts = jnp.concatenate([line.astype(F32) for line in split3(res_rows[...])], axis=0)
    found = mm(parts.astype(BF16), is_lane)
    found = found[: 2 * O] + found[2 * O : 4 * O] + found[4 * O :]
    mask = iota((O, L), 0) == block_i * C + ahead
    out_ref[0:1, :L] = jnp.sum(jnp.where(mask, found[:O], 0.0), axis=0, keepdims=True)
    out_ref[1:2, :L] = jnp.sum(jnp.where(mask, found[O:], 0.0), axis=0, keepdims=True)


def local(documents, assigned, centroids, owner_slot):
    L, D = documents.shape
    S = centroids.shape[0]
    R = lax.axis_size("dp")
    C = lax.axis_size("cent")
    O = R * C
    pair_cap = 2 * L // O
    row_cap = 5 * C * pair_cap // 8
    K = round_up(pair_cap, 16)
    Q = round_up(row_cap, 16)
    CK = C * K
    QP = round_up(Q, LANES)
    half, unit = D // 2, D // 8
    cuts = [(half, half)] * (R - 2) + [(2 * unit,) * 4, (2 * unit,) * 3 + (unit,) * 2]
    copies = sum(len(c) for c in cuts) if R <= 8 else R
    T = owner_slot.shape[0] // LANES
    hbm = pl.BlockSpec(memory_space=pl.ANY)
    dma = pltpu.SemaphoreType.DMA
    packed = pl.pallas_call(
        functools.partial(kernel, (R, C, K, Q, cuts)),
        name="cluster_exchange",
        out_shape=pltpu.VMEM((SUB, max(L, S)), F32),
        in_specs=[hbm] * 4,
        out_specs=pl.BlockSpec(memory_space=pltpu.VMEM),
        scratch_shapes=[
            pltpu.VMEM((L, D), BF16),
            pltpu.VMEM((1, L), jnp.int32),
            pltpu.VMEM((T, LANES), jnp.int32),
            pltpu.VMEM((S + R * CK, D), BF16),
            pltpu.VMEM((R, Q, D), BF16),
            pltpu.VMEM((R, Q, D), BF16),
            pltpu.VMEM((R, 2, QP), F32),
            pltpu.VMEM((R, 2, QP), F32),
            pltpu.VMEM((R, C - 1, K, D), BF16),
            pltpu.VMEM((R, 1, LANES), F32),
            pltpu.VMEM((R, C, 1, LANES), F32),
            pltpu.VMEM((R, 2, LANES), F32),
            pltpu.VMEM((O, 2, LANES), F32),
            pltpu.VMEM((2 * O, LANES), F32),
            pltpu.VMEM((R, 1, CK), F32),
            pltpu.VMEM((R, CK, CK), F32),
            pltpu.VMEM((R, 1, CK), F32),
            pltpu.VMEM((R, CK, CK), F32),
            pltpu.VMEM((R, 1, CK), F32),
            pltpu.VMEM((R, 1, CK), F32),
            pltpu.VMEM((R, CK, CK), F32),
            pltpu.VMEM((S, CK), F32),
            pltpu.VMEM((S + R * CK if R <= 8 else SUB, CK), F32),
            pltpu.VMEM((SUB, S), F32),
            dma((4,)),
            dma((1,)),
            dma((copies,)),
            dma((1,)),
            dma((1,)),
            dma((1,)),
            dma((copies,)),
            dma((1,)),
            dma((R,)),
            dma((1,)),
            dma((1,)),
        ],
        compiler_params=pltpu.CompilerParams(
            collective_id=0, has_side_effects=True, vmem_limit_bytes=62 * 1024 * 1024
        ),
    )(
        documents,
        assigned.reshape(1, L),
        centroids,
        owner_slot.reshape(-1, LANES),
    )
    return packed[0, :L], packed[1, :L], packed[2:5, :S]


def solution(mesh):
    in_specs = (P(("dp", "cent"), None), P(("dp", "cent")), P(("dp", "cent"), None), P())
    out_specs = (P(("dp", "cent")), P(("dp", "cent")), P(None, ("dp", "cent")))
    return jax.shard_map(local, mesh=mesh, in_specs=in_specs, out_specs=out_specs, check_vma=False)
```

```python
import functools
import math

import jax
import jax.numpy as jnp
from jax import lax
from jax.experimental import pallas as pl
from jax.experimental.pallas import tpu as pltpu
from jax.sharding import PartitionSpec as P

F32 = jnp.float32
BF16 = jnp.bfloat16
LANES = 128
SUB = 8


def round_up(value, unit):
    return -(-value // unit) * unit


def each(low, high, body):
    if high - low <= 8:
        for step in range(low, high):
            body(step)
    else:
        lax.fori_loop(low, high, lambda step, carry: (body(step), carry)[1], 0)


def iota(shape, dim):
    return lax.broadcasted_iota(jnp.int32, shape, dim)


def mm(left, right):
    return lax.dot_general(left, right, (((1,), (0,)), ((), ())), preferred_element_type=F32)


def mm_t(left, right):
    return lax.dot_general(left, right, (((1,), (1,)), ((), ())), preferred_element_type=F32)


def one_hot(condition):
    return jnp.where(condition, 1.0, 0.0).astype(BF16)


def split3(value):
    high = value.astype(BF16)
    rest = value - high.astype(F32)
    mid = rest.astype(BF16)
    low = (rest - mid.astype(F32)).astype(BF16)
    return high, mid, low


def kernel(
    dims,
    docs_hbm,
    assigned_hbm,
    cent_hbm,
    table_hbm,
    out_ref,
    docs_ref,
    assigned_ref,
    table_ref,
    all_buf,
    send_buf,
    chunk_buf,
    code_send,
    code_recv,
    fwd_buf,
    dir_buf,
    tag_send,
    tag_recv,
    res_send,
    res_recv,
    res_rows,
    tag_row,
    tag_mat,
    inv_row,
    inv_mat,
    sim_row,
    best_row,
    best_mat,
    cent_mat,
    gram_acc,
    stats_ref,
    in_sem,
    a_send,
    a_recv,
    m_send,
    m_recv,
    f_send,
    f_recv,
    t_send,
    t_recv,
    r_send,
    r_recv,
    d_send,
):
    R, C, K, Q, cuts = dims
    O = R * C
    CK = C * K
    L, D = docs_ref.shape
    S = cent_hbm.shape[0]
    T = table_ref.shape[0]
    QP = code_send.shape[2]
    small = R <= 8
    direct = R == 8
    row_me = lax.axis_index("dp")
    col_me = lax.axis_index("cent")
    own = row_me * C + col_me

    bits = []
    while 2 ** len(bits) < R:
        bits.append(lax.rem(lax.div(row_me, 2 ** len(bits)), 2))
    col_of = [col_me] + [lax.rem(col_me + d, C) for d in range(1, C)]

    swap = {3: 4, 4: 3} if R == 8 else {}

    def row_of(t):
        total = 0
        if isinstance(t, int):
            t = swap.get(t, t)
        for i, bit in enumerate(bits):
            if isinstance(t, int):
                total = total + (1 - bit if (t >> i) & 1 else bit) * 2**i
            else:
                total = total + lax.rem(bit + lax.div(t, 2**i), 2) * 2**i
        return total

    def all_peers(body):
        def at_row(t):
            r = row_of(t)
            for d in range(C):
                body(t, r, d)

        each(1, R, at_row)
        for d in range(1, C):
            body(0, row_me, d)

    def where_is(r, c):
        return {"dp": r, "cent": c}

    def remote(src, dst, send, recv, r, c):
        return pltpu.make_async_remote_copy(
            src_ref=src,
            dst_ref=dst,
            send_sem=send,
            recv_sem=recv,
            device_id=where_is(r, c),
            device_id_type=pl.DeviceIdType.MESH,
        )

    barrier = pltpu.get_barrier_semaphore()

    def greet(r, c):
        pl.semaphore_signal(
            barrier, inc=1, device_id=where_is(r, c), device_id_type=pl.DeviceIdType.MESH
        )

    each(1, R, lambda t: greet(row_of(t), col_me))
    for d in range(1, C):
        greet(row_me, col_of[d])

    cent_rows = all_buf.at[pl.ds(0, S), :]
    loads = [
        pltpu.make_async_copy(assigned_hbm, assigned_ref, in_sem.at[0]),
        pltpu.make_async_copy(table_hbm, table_ref, in_sem.at[1]),
        pltpu.make_async_copy(docs_hbm, docs_ref, in_sem.at[2]),
        pltpu.make_async_copy(cent_hbm, cent_rows, in_sem.at[3]),
    ]
    for load in loads:
        load.start()
    loads[0].wait()
    loads[1].wait()

    assigned = assigned_ref[...]
    high = lax.shift_right_logical(assigned, 7)
    low = jnp.bitwise_and(assigned, 127)
    table = table_ref[...]
    pick = one_hot(iota((T, L), 0) == high)
    looked = jnp.zeros((LANES, L), F32)
    shift = 0
    while 2**shift < O * S:
        digit = jnp.bitwise_and(lax.shift_right_logical(table, shift), 255)
        looked = looked + float(2**shift) * lax.dot_general(
            digit.astype(F32).astype(BF16), pick, (((0,), (0,)), ((), ())), preferred_element_type=F32
        )
        shift += 8
    slot = jnp.sum(jnp.where(iota((LANES, L), 0) == low, looked, 0.0), axis=0, keepdims=True)
    owner = jnp.floor((slot + 0.5) * (1.0 / S))
    row = jnp.floor((owner + 0.5) * (1.0 / C))
    owner_i = owner.astype(jnp.int32)
    row_i = row.astype(jnp.int32)
    cent_i = owner_i - row_i * C
    is_owner = jnp.where(iota((O, L), 0) == owner_i, 1.0, 0.0)
    is_row = jnp.where(iota((R, L), 0) == row_i, 1.0, 0.0)
    earlier = one_hot(iota((L, L), 0) < iota((L, L), 1))
    ranks = mm(jnp.concatenate([is_owner, is_row], axis=0).astype(BF16), earlier)
    rank_owner = jnp.sum(ranks[:O] * is_owner, axis=0, keepdims=True)
    rank_row = jnp.sum(ranks[O:] * is_row, axis=0, keepdims=True)
    block_i = jnp.bitwise_xor(row_i, row_me)
    if swap:
        block_i = jnp.where((block_i == 3) | (block_i == 4), 7 - block_i, block_i)
    position = block_i * Q + rank_row.astype(jnp.int32)
    rank_i = rank_owner.astype(jnp.int32)

    ahead = cent_i - col_me
    ahead = jnp.where(ahead < 0, ahead + C, ahead)
    behind = jnp.where(ahead == 0, 0, C - ahead)
    lane_i = behind * K + rank_i
    is_lane = one_hot(iota((LANES, L), 0) == lane_i)

    tag = slot - owner * S + 1.0
    tag_hi = jnp.floor(tag * (1.0 / 128.0))
    lines = jnp.concatenate(
        [(ahead * K + rank_i + 1).astype(F32), tag_hi, tag - tag_hi * 128.0, jnp.zeros((SUB - 3, L), F32)],
        axis=0,
    ).astype(BF16)

    def mark(t):
        here = jnp.where(position < (t + 1) * Q, position, -1)
        line = mm_t(lines, one_hot(iota((QP, L), 0) + t * Q == here))
        code_send[t, 0:1, :] = line[0:1]
        code_send[t, 1:2, :] = 128.0 * line[1:2] + line[2:3]

    each(0, R, mark)

    def cut(t, p):
        width = cuts[t][p] if small else D
        return pl.ds(sum(cuts[t][:p]) if small else 0, width), width

    def sem(t, p):
        return sum(len(c) for c in cuts[:t]) + p if small else t

    def pieces(t):
        return range(len(cuts[t])) if small else range(1)

    def ends(t, p):
        return int(direct and t == R - 1 and p == len(cuts[t]) - 1)

    def row_copy(t, p):
        at = cut(t, p)[0]
        return remote(
            send_buf.at[t, :, at], chunk_buf.at[t, :, at], a_send.at[ends(t, p)], a_recv.at[sem(t, p)], row_of(t), col_me
        )

    def code_copy(t):
        return remote(code_send.at[t], code_recv.at[t], m_send.at[0], m_recv.at[t], row_of(t), col_me)

    def whole(ref, send, recv):
        return remote(ref, ref, send.at[0], recv.at[0], row_of(1), col_me)


    def start_rows(t):
        for p in pieces(t):
            if not ends(t, p):
                row_copy(t, p).start()

    def rows_at(t, block=0, count=None):
        return pl.ds(S + t * CK + block * K, CK if count is None else count)

    def dir_copy(d):
        return remote(
            dir_buf.at[d],
            all_buf.at[rows_at(7, (C - d) % C, K), cut(7, len(cuts[7]) - 1)[0]],
            d_send.at[0],
            f_recv.at[sem(7, len(cuts[7]) - 1)],
            row_of(7),
            col_of[d],
        )

    def choose(ts):
        wanted = [one_hot(iota((Q, L), 0) + t * Q == position) for t in ts]
        found = mm(jnp.concatenate(wanted, axis=0), docs_ref[...]).astype(BF16)
        for i, t in enumerate(ts):
            send_buf[t] = found[i * Q : (i + 1) * Q]

    def first_sends():
        pl.semaphore_wait(barrier, R + C - 2)
        each(1, R, lambda t: code_copy(t).start())

    loads[2].wait()
    if R == 8:
        inner = lax.rem(bits[-1] + bits[-2], 2) == 1
        choose([3, 1])
        first_sends()

        @pl.when(inner)
        def _():
            start_rows(3)

        start_rows(1)
        choose([2, 4])
        start_rows(2)
        start_rows(4)

        @pl.when(jnp.logical_not(inner))
        def _():
            start_rows(3)

        choose([5, 6])
        start_rows(5)
        start_rows(6)
        choose([7, 0])
        start_rows(7)
        final = len(cuts[7]) - 1

        @pl.when(inner)
        def _():
            wanted = one_hot(iota((CK, L), 0) == jnp.where(block_i == 7, ahead * K + rank_i, -1))
            found = mm(wanted, docs_ref[:, D - cuts[7][final] :]).astype(BF16)
            dir_buf[...] = found.reshape(dir_buf.shape)

        @pl.when(jnp.logical_not(inner))
        def _():
            row_copy(7, final).start()
    else:
        first_sends()
        group = max(1, R // 2)
        for first in range(0, R, group):
            wanted = one_hot(iota((group * Q, L), 0) + first * Q == position)
            send_buf[first : first + group] = (
                mm(wanted, docs_ref[...]).astype(BF16).reshape(group, Q, D)
            )
            each(max(first, 1), first + group, start_rows)

    def fwd_copy(t, d, p):
        at = cut(t, p)[0]
        return remote(
            fwd_buf.at[t, d - 1, :, at],
            all_buf.at[rows_at(t, C - d, K), at],
            f_send.at[ends(t, p)],
            f_recv.at[sem(t, p)],
            row_me,
            col_of[d],
        )

    def fwd_arrival(t, p):
        ref = all_buf.at[rows_at(t, 1, CK - K), cut(t, p)[0]]
        return remote(ref, ref, f_send.at[0], f_recv.at[sem(t, p)], row_me, col_of[1])

    def dir_arrival(t, p):
        ref = all_buf.at[rows_at(t), cut(t, p)[0]]
        return remote(ref, ref, d_send.at[0], f_recv.at[sem(t, p)], row_me, col_of[1])

    def tag_copy(t, d):
        return remote(
            tag_send.at[t], tag_recv.at[t, C - d], t_send.at[0], t_recv.at[t], row_me, col_of[d]
        )

    def tag_arrival(t):
        ref = tag_recv.at[t, pl.ds(1, C - 1)]
        return remote(ref, ref, t_send.at[0], t_recv.at[t], row_me, col_of[1])

    block = iota((CK, Q), 0) // K
    turned = jnp.where(block == 0, 0, C - block) * K + iota((CK, Q), 0) - block * K + 1

    def relay(t, p, mine=False):
        if ends(t, p):
            pl.when(jnp.logical_not(inner))(lambda: relay_now(t, p))
        else:
            relay_now(t, p, mine)

    def relay_now(t, p, mine=False):
        if not mine:
            if p == 0 and direct and t == R - 1:
                pl.when(jnp.logical_not(inner))(lambda: code_copy(t).wait_recv())
            elif p == 0:
                code_copy(t).wait_recv()
            row_copy(t, p).wait_recv()
        at, width = cut(t, p)
        lines = (code_send if mine else code_recv)[t][:, :Q]
        line = lines[0:1].astype(jnp.int32)
        wanted = one_hot(iota((CK, Q), 0) + 1 == line)
        if p == 0:
            high = jnp.floor(lines[1:2] * (1.0 / 128.0))
            digits = [high, lines[1:2] - high * 128.0, jnp.zeros((SUB - 2, Q), F32)]
            digits = mm_t(jnp.concatenate(digits, axis=0).astype(BF16), one_hot(turned == line))
            tag_send[t, 0:1, :CK] = 128.0 * digits[0:1] + digits[1:2]
            for d in range(1, C):
                tag_copy(t, d).start()
        found = mm(wanted, (send_buf if mine else chunk_buf)[t, :, at]).astype(BF16)
        fwd_buf[t, :, :, at] = found[K:].reshape(C - 1, K, width)
        for d in range(1, C):
            fwd_copy(t, d, p).start()
        all_buf[rows_at(t, 0, K), at] = found[:K]

    if CK < LANES:
        tag_send[...] = jnp.zeros(tag_send.shape, F32)
    for p in pieces(0):
        relay(0, p, True)

    loads[3].wait()
    norm = jnp.zeros((S, LANES), F32)
    for part in range(0, D, LANES):
        block = all_buf[0:S, part : part + LANES].astype(F32)
        norm = norm + block * block
    cent_mat[...] = jnp.broadcast_to(
        lax.rsqrt(jnp.sum(norm, axis=1, keepdims=True) + 1.0), cent_mat.shape
    )


    eye = iota((CK, CK), 0) == iota((CK, CK), 1)

    def spread(t):
        tag_arrival(t).wait_recv()
        line = tag_send[t][:, :CK]
        for c in range(1, C):
            line = jnp.where(iota((1, CK), 1) // K == c, tag_recv[t, c][:, :CK], line)
        tag_row[t] = line
        tag_mat[t] = jnp.broadcast_to(
            jnp.sum(jnp.where(eye, line, 0.0), axis=1, keepdims=True), (CK, CK)
        )
        best_mat[t] = jnp.zeros((CK, CK), F32)

    stats_ref[...] = jnp.zeros(stats_ref.shape, F32)

    def member_of(t):
        return (iota((S, CK), 0) + 1).astype(F32) == tag_row[t]

    def self_block(t, gram):
        diag = jnp.where(eye, gram, 0.0)
        row_scale = lax.rsqrt(jnp.sum(diag, axis=0, keepdims=True) + 1.0)
        col_scale = lax.rsqrt(jnp.sum(diag, axis=1, keepdims=True) + 1.0)
        inv_row[t] = row_scale
        inv_mat[t] = jnp.broadcast_to(col_scale, (CK, CK))
        line = jnp.where(tag_row[t] > 0.0, tag_row[t], -1.0)
        same = (tag_mat[t] == line) & jnp.logical_not(eye)
        best = jnp.max(jnp.where(same, gram * col_scale, 0.0), axis=0, keepdims=True)
        return row_scale, line, best

    def other_block(u, gram, row_scale, line, best):
        same = tag_mat[u] == line
        best_mat[u] = jnp.maximum(best_mat[u], jnp.where(same, gram * row_scale, 0.0))
        return jnp.maximum(
            best, jnp.max(jnp.where(same, gram * inv_mat[u], 0.0), axis=0, keepdims=True)
        )

    def cross_block(t, cross, row_scale):
        member = member_of(t)
        similarity = row_scale * jnp.sum(
            jnp.where(member, cross * cent_mat[...], 0.0), axis=0, keepdims=True
        )
        sim_row[t] = similarity
        lines = [jnp.ones((1, CK), BF16), *split3(similarity), *split3(similarity * similarity)]
        lines = jnp.concatenate(
            [line.astype(F32) for line in lines] + [jnp.zeros((1, CK), F32)], axis=0
        )
        stats_ref[...] += mm_t(lines.astype(BF16), one_hot(member))

    def settle(t, read):
        row_scale, line, best = self_block(t, read(S + t * CK, CK))
        for u in range(t):
            best = other_block(u, read(S + u * CK, CK), row_scale, line, best)
        best_row[t] = best
        cross_block(t, read(0, S), row_scale)

    def arrivals(t, p):
        if ends(t, p):

            @pl.when(inner)
            def _():
                dir_arrival(t, p).wait_recv()

            @pl.when(jnp.logical_not(inner))
            def _():
                fwd_arrival(t, p).wait_recv()

        else:
            fwd_arrival(t, p).wait_recv()

    def absorb_piece(t, p):
        if p == 0:
            spread(t)
        arrivals(t, p)
        at = cut(t, p)[0]
        rows = S + (t + 1) * CK
        before = gram_acc[0:rows] if p else None
        part = mm_t(all_buf[0:rows, at], all_buf[rows_at(t), at])
        gram_acc[0:rows] = part if p == 0 else before + part
        if p == len(cuts[t]) - 1:
            settle(t, lambda start, count: gram_acc[start : start + count])

    def absorb_last():
        t = R - 1
        n = len(cuts[t])
        width = cuts[t][0]
        rows = S + R * CK
        spread(t)

        def step(p, carry):
            at = pl.ds(pl.multiple_of(p * width, width), width)
            semaphore = f_recv.at[sem(t, 0) + p]
            straight = jnp.logical_and(inner, p == n - 1)

            @pl.when(straight)
            def _():
                ref = all_buf.at[rows_at(t), at]
                remote(ref, ref, d_send.at[0], semaphore, row_me, col_of[1]).wait_recv()

            @pl.when(jnp.logical_not(straight))
            def _():
                ref = all_buf.at[rows_at(t, 1, CK - K), at]
                remote(ref, ref, d_send.at[0], semaphore, row_me, col_of[1]).wait_recv()

            before = jnp.where(p > 0, gram_acc[0:rows], 0.0)
            gram_acc[0:rows] = before + mm_t(all_buf[0:rows, at], all_buf[rows_at(t), at])
            return carry

        lax.fori_loop(0, n, step, 0)
        settle(t, lambda start, count: gram_acc[start : start + count])

    def absorb(t):
        for p in pieces(t):
            absorb_piece(t, p)

    def absorb_any(t):
        spread(t)
        arrivals(t, 0)
        mine = all_buf[rows_at(t), :]
        row_scale, line, best = self_block(t, mm_t(mine, mine))

        def pair(u, best):
            return other_block(u, mm_t(all_buf[rows_at(u), :], mine), row_scale, line, best)

        best_row[t] = lax.fori_loop(0, t, pair, best)
        cross_block(t, mm_t(all_buf[0:S, :], mine), row_scale)

    def relay_all(*ts):
        for p in pieces(ts[0]):
            for t in ts:
                relay(t, p)

    if R == 8:
        relay_all(1)

        @pl.when(inner)
        def _():
            code_copy(7).wait_recv()
            for d in range(C):
                dir_copy(d).start()

        absorb(0)
        relay_all(2, 3)
        absorb(1)
        relay(4, 0)
        relay(5, 0)
        absorb(2)
        relay(4, 1)
        relay(5, 1)
        absorb(3)
        absorb(4)
        absorb(5)
        steps = [(t, p) for t in (6, 7) for p in pieces(t)]
        lag = 3
        for i in range(-lag, len(cuts[6])):
            relay(*steps[i + lag])
            if i >= 0:
                absorb_piece(*steps[i])
        for step in steps[len(cuts[6]) + lag :]:
            relay(*step)
        absorb_last()
    elif small:
        for t in range(1, R):
            relay_all(t)
            absorb(t - 1)
        absorb(R - 1)
    else:

        def advance(t, carry):
            relay_all(t)
            absorb_any(t - 1)
            return carry

        lax.fori_loop(1, R, advance, 0)
        absorb_any(R - 1)

    stats = stats_ref[...]
    count = stats[0:1]
    total = stats[1:2] + stats[2:3] + stats[3:4]
    square = stats[4:5] + stats[5:6] + stats[6:7]
    floor = jnp.maximum(count, 1.0)
    mean = total / floor
    variance = jnp.maximum(square / floor - mean * mean, 0.0)
    spread_inv = 1.0 / jnp.sqrt(variance + 1.0 / D)
    wanted = [line.astype(F32) for line in (*split3(mean), *split3(spread_inv))]
    wanted = jnp.concatenate(wanted + [jnp.zeros((2, S), F32)], axis=0).astype(BF16)

    def res_copy(t, r, d):
        return remote(
            res_send.at[t], res_recv.at[t * C + (C - d) % C], r_send.at[0], r_recv.at[0], r, col_of[d]
        )

    res_all = whole(res_recv.at[pl.ds(1, O - 1)], r_send, r_recv)

    def finish(t, found):
        centre = found[0:1] + found[1:2] + found[2:3]
        width = found[3:4] + found[4:5] + found[5:6]
        proto = (centre - sim_row[t]) * width
        column = jnp.max(best_mat[t], axis=1, keepdims=True)
        flat = jnp.max(jnp.where(eye, column, 0.0), axis=0, keepdims=True)
        redundant = jnp.maximum(flat, best_row[t]) * inv_row[t] * math.sqrt(D)
        res_send[t, 0:1, :CK] = proto
        res_send[t, 1:2, :CK] = redundant

    if CK < LANES:
        res_send[...] = jnp.zeros(res_send.shape, F32)

    def deliver(t):
        r = row_of(t)
        for d in (2, 3, 1, 0) if C == 4 else range(C):
            if not (isinstance(t, int) and t == 0 and d == 0):
                res_copy(t, r, d).start()

    if small:
        members = jnp.concatenate([one_hot(member_of(t)) for t in range(R)], axis=1)
        found = mm(wanted, members)
        for t in range(R):
            finish(t, found[:, t * CK : (t + 1) * CK])
        for t in [5, 3, 7, 6, 4, 2, 1, 0] if R == 8 else range(R):
            deliver(t)
    else:

        def finish_any(t):
            finish(t, mm(wanted, one_hot(member_of(t))))

        each(0, R, finish_any)
        each(1, R, deliver)
        deliver(0)
    res_recv[0] = res_send[0]
    out_ref[2:3, :S] = count
    out_ref[3:4, :S] = total
    out_ref[4:5, :S] = square

    def sent(ref, semaphore):
        remote(ref, ref, semaphore, r_recv.at[0], row_me, col_of[1]).wait_send()

    if direct:
        kept = D - cuts[-1][-1]
        sent(send_buf.at[pl.ds(1, R - 2)], a_send.at[0])
        sent(send_buf.at[R - 1, :, pl.ds(0, kept)], a_send.at[0])
        sent(fwd_buf.at[pl.ds(0, R - 1)], f_send.at[0])
        sent(fwd_buf.at[R - 1, :, :, pl.ds(0, kept)], f_send.at[0])

        @pl.when(inner)
        def _():
            sent(dir_buf, d_send.at[0])

        @pl.when(jnp.logical_not(inner))
        def _():
            sent(send_buf.at[R - 1, :, pl.ds(kept, D - kept)], a_send.at[1])
            sent(fwd_buf.at[R - 1, :, :, pl.ds(kept, D - kept)], f_send.at[1])

    else:
        sent(send_buf.at[pl.ds(1, R - 1)], a_send.at[0])
        sent(fwd_buf, f_send.at[0])
    sent(code_recv.at[pl.ds(1, R - 1)], m_send.at[0])
    sent(tag_recv.at[:, pl.ds(1, C - 1)], t_send.at[0])
    res_all.wait_send()
    res_all.wait_recv()

    for o in range(O):
        pair = res_recv[o]
        res_rows[o : o + 1, :] = pair[0:1]
        res_rows[O + o : O + o + 1, :] = pair[1:2]
    parts = jnp.concatenate([line.astype(F32) for line in split3(res_rows[...])], axis=0)
    found = mm(parts.astype(BF16), is_lane)
    found = found[: 2 * O] + found[2 * O : 4 * O] + found[4 * O :]
    mask = iota((O, L), 0) == block_i * C + ahead
    out_ref[0:1, :L] = jnp.sum(jnp.where(mask, found[:O], 0.0), axis=0, keepdims=True)
    out_ref[1:2, :L] = jnp.sum(jnp.where(mask, found[O:], 0.0), axis=0, keepdims=True)


def local(documents, assigned, centroids, owner_slot):
    L, D = documents.shape
    S = centroids.shape[0]
    R = lax.axis_size("dp")
    C = lax.axis_size("cent")
    O = R * C
    pair_cap = 2 * L // O
    row_cap = 5 * C * pair_cap // 8
    K = round_up(pair_cap, 16)
    Q = round_up(row_cap, 16)
    CK = C * K
    QP = round_up(Q, LANES)
    half, unit = D // 2, D // 8
    cuts = [(half, half)] * (R - 2) + [(2 * unit,) * 4] * 2
    copies = sum(len(c) for c in cuts) if R <= 8 else R
    T = owner_slot.shape[0] // LANES
    hbm = pl.BlockSpec(memory_space=pl.ANY)
    dma = pltpu.SemaphoreType.DMA
    packed = pl.pallas_call(
        functools.partial(kernel, (R, C, K, Q, cuts)),
        name="cluster_exchange",
        out_shape=pltpu.VMEM((SUB, max(L, S)), F32),
        in_specs=[hbm] * 4,
        out_specs=pl.BlockSpec(memory_space=pltpu.VMEM),
        scratch_shapes=[
            pltpu.VMEM((L, D), BF16),
            pltpu.VMEM((1, L), jnp.int32),
            pltpu.VMEM((T, LANES), jnp.int32),
            pltpu.VMEM((S + R * CK, D), BF16),
            pltpu.VMEM((R, Q, D), BF16),
            pltpu.VMEM((R, Q, D), BF16),
            pltpu.VMEM((R, 2, QP), F32),
            pltpu.VMEM((R, 2, QP), F32),
            pltpu.VMEM((R, C - 1, K, D), BF16),
            pltpu.VMEM((C, K, cuts[-1][-1]), BF16),
            pltpu.VMEM((R, 1, LANES), F32),
            pltpu.VMEM((R, C, 1, LANES), F32),
            pltpu.VMEM((R, 2, LANES), F32),
            pltpu.VMEM((O, 2, LANES), F32),
            pltpu.VMEM((2 * O, LANES), F32),
            pltpu.VMEM((R, 1, CK), F32),
            pltpu.VMEM((R, CK, CK), F32),
            pltpu.VMEM((R, 1, CK), F32),
            pltpu.VMEM((R, CK, CK), F32),
            pltpu.VMEM((R, 1, CK), F32),
            pltpu.VMEM((R, 1, CK), F32),
            pltpu.VMEM((R, CK, CK), F32),
            pltpu.VMEM((S, CK), F32),
            pltpu.VMEM((S + R * CK if R <= 8 else SUB, CK), F32),
            pltpu.VMEM((SUB, S), F32),
            dma((4,)),
            dma((2,)),
            dma((copies,)),
            dma((1,)),
            dma((R,)),
            dma((2,)),
            dma((copies,)),
            dma((1,)),
            dma((R,)),
            dma((1,)),
            dma((1,)),
            dma((1,)),
        ],
        compiler_params=pltpu.CompilerParams(
            collective_id=0, has_side_effects=True, vmem_limit_bytes=62 * 1024 * 1024
        ),
    )(
        documents,
        assigned.reshape(1, L),
        centroids,
        owner_slot.reshape(-1, LANES),
    )
    return packed[0, :L], packed[1, :L], packed[2:5, :S]


def solution(mesh):
    in_specs = (P(("dp", "cent"), None), P(("dp", "cent")), P(("dp", "cent"), None), P())
    out_specs = (P(("dp", "cent")), P(("dp", "cent")), P(None, ("dp", "cent")))
    return jax.shard_map(local, mesh=mesh, in_specs=in_specs, out_specs=out_specs, check_vma=False)
```

```python
import functools
import math

import jax
import jax.numpy as jnp
from jax import lax
from jax.experimental import pallas as pl
from jax.experimental.pallas import tpu as pltpu
from jax.sharding import PartitionSpec as P

F32 = jnp.float32
BF16 = jnp.bfloat16
LANES = 128
SUB = 8


def round_up(value, unit):
    return -(-value // unit) * unit


def each(low, high, body):
    if high - low <= 8:
        for step in range(low, high):
            body(step)
    else:
        lax.fori_loop(low, high, lambda step, carry: (body(step), carry)[1], 0)


def iota(shape, dim):
    return lax.broadcasted_iota(jnp.int32, shape, dim)


def mm(left, right):
    return lax.dot_general(left, right, (((1,), (0,)), ((), ())), preferred_element_type=F32)


def mm_t(left, right):
    return lax.dot_general(left, right, (((1,), (1,)), ((), ())), preferred_element_type=F32)


def one_hot(condition):
    return jnp.where(condition, 1.0, 0.0).astype(BF16)


def split3(value):
    high = value.astype(BF16)
    rest = value - high.astype(F32)
    mid = rest.astype(BF16)
    low = (rest - mid.astype(F32)).astype(BF16)
    return high, mid, low


def kernel(
    dims,
    docs_hbm,
    assigned_hbm,
    cent_hbm,
    table_hbm,
    out_ref,
    docs_ref,
    assigned_ref,
    table_ref,
    all_buf,
    send_buf,
    chunk_buf,
    code_send,
    code_recv,
    fwd_buf,
    dir_buf,
    tag_send,
    tag_recv,
    res_send,
    res_recv,
    res_rows,
    tag_row,
    tag_mat,
    inv_row,
    inv_mat,
    sim_row,
    best_row,
    best_mat,
    cent_mat,
    gram_acc,
    stats_ref,
    in_sem,
    a_send,
    a_recv,
    m_send,
    m_recv,
    f_send,
    f_recv,
    t_send,
    t_recv,
    r_send,
    r_recv,
    d_send,
):
    R, C, K, Q, cuts, straight = dims
    tail = straight * cuts[-1][-1]
    O = R * C
    CK = C * K
    L, D = docs_ref.shape
    S = cent_hbm.shape[0]
    T = table_ref.shape[0]
    QP = code_send.shape[2]
    small = R <= 8
    direct = R == 8
    row_me = lax.axis_index("dp")
    col_me = lax.axis_index("cent")
    own = row_me * C + col_me

    bits = []
    while 2 ** len(bits) < R:
        bits.append(lax.rem(lax.div(row_me, 2 ** len(bits)), 2))
    col_of = [col_me] + [lax.rem(col_me + d, C) for d in range(1, C)]

    plan = [0, 1, 2, 3, -1, 100, 101, -2, 102, 103, -3, 104, -4]

    swap = {3: 4, 4: 3} if R == 8 else {}

    def row_of(t):
        total = 0
        if isinstance(t, int):
            t = swap.get(t, t)
        for i, bit in enumerate(bits):
            if isinstance(t, int):
                total = total + (1 - bit if (t >> i) & 1 else bit) * 2**i
            else:
                total = total + lax.rem(bit + lax.div(t, 2**i), 2) * 2**i
        return total

    def all_peers(body):
        def at_row(t):
            r = row_of(t)
            for d in range(C):
                body(t, r, d)

        each(1, R, at_row)
        for d in range(1, C):
            body(0, row_me, d)

    def where_is(r, c):
        return {"dp": r, "cent": c}

    def remote(src, dst, send, recv, r, c):
        return pltpu.make_async_remote_copy(
            src_ref=src,
            dst_ref=dst,
            send_sem=send,
            recv_sem=recv,
            device_id=where_is(r, c),
            device_id_type=pl.DeviceIdType.MESH,
        )

    barrier = pltpu.get_barrier_semaphore()

    def greet(r, c):
        pl.semaphore_signal(
            barrier, inc=1, device_id=where_is(r, c), device_id_type=pl.DeviceIdType.MESH
        )

    each(1, R, lambda t: greet(row_of(t), col_me))
    for d in range(1, C):
        greet(row_me, col_of[d])

    cent_rows = all_buf.at[pl.ds(0, S), :]
    loads = [
        pltpu.make_async_copy(assigned_hbm, assigned_ref, in_sem.at[0]),
        pltpu.make_async_copy(table_hbm, table_ref, in_sem.at[1]),
        pltpu.make_async_copy(docs_hbm, docs_ref, in_sem.at[2]),
        pltpu.make_async_copy(cent_hbm, cent_rows, in_sem.at[3]),
    ]
    for load in loads:
        load.start()
    loads[0].wait()
    loads[1].wait()

    assigned = assigned_ref[...]
    high = lax.shift_right_logical(assigned, 7)
    low = jnp.bitwise_and(assigned, 127)
    table = table_ref[...]
    pick = one_hot(iota((T, L), 0) == high)
    looked = jnp.zeros((LANES, L), F32)
    shift = 0
    while 2**shift < O * S:
        digit = jnp.bitwise_and(lax.shift_right_logical(table, shift), 255)
        looked = looked + float(2**shift) * lax.dot_general(
            digit.astype(F32).astype(BF16), pick, (((0,), (0,)), ((), ())), preferred_element_type=F32
        )
        shift += 8
    slot = jnp.sum(jnp.where(iota((LANES, L), 0) == low, looked, 0.0), axis=0, keepdims=True)
    owner = jnp.floor((slot + 0.5) * (1.0 / S))
    row = jnp.floor((owner + 0.5) * (1.0 / C))
    owner_i = owner.astype(jnp.int32)
    row_i = row.astype(jnp.int32)
    cent_i = owner_i - row_i * C
    is_owner = jnp.where(iota((O, L), 0) == owner_i, 1.0, 0.0)
    is_row = jnp.where(iota((R, L), 0) == row_i, 1.0, 0.0)
    earlier = one_hot(iota((L, L), 0) < iota((L, L), 1))
    ranks = mm(jnp.concatenate([is_owner, is_row], axis=0).astype(BF16), earlier)
    rank_owner = jnp.sum(ranks[:O] * is_owner, axis=0, keepdims=True)
    rank_row = jnp.sum(ranks[O:] * is_row, axis=0, keepdims=True)
    block_i = jnp.bitwise_xor(row_i, row_me)
    if swap:
        block_i = jnp.where((block_i == 3) | (block_i == 4), 7 - block_i, block_i)
    position = block_i * Q + rank_row.astype(jnp.int32)
    rank_i = rank_owner.astype(jnp.int32)

    ahead = cent_i - col_me
    ahead = jnp.where(ahead < 0, ahead + C, ahead)
    behind = jnp.where(ahead == 0, 0, C - ahead)
    lane_i = behind * K + rank_i
    is_lane = one_hot(iota((LANES, L), 0) == lane_i)

    tag = slot - owner * S + 1.0
    tag_hi = jnp.floor(tag * (1.0 / 128.0))
    lines = jnp.concatenate(
        [(ahead * K + rank_i + 1).astype(F32), tag_hi, tag - tag_hi * 128.0, jnp.zeros((SUB - 3, L), F32)],
        axis=0,
    ).astype(BF16)

    def mark(t):
        here = jnp.where(position < (t + 1) * Q, position, -1)
        line = mm_t(lines, one_hot(iota((QP, L), 0) + t * Q == here))
        code_send[t, 0:1, :] = line[0:1]
        code_send[t, 1:2, :] = 128.0 * line[1:2] + line[2:3]

    each(0, R, mark)

    def cut(t, p):
        width = cuts[t][p] if small else D
        return pl.ds(sum(cuts[t][:p]) if small else 0, width), width

    def sem(t, p):
        return sum(len(c) for c in cuts[:t]) + p if small else t

    def pieces(t):
        return range(len(cuts[t])) if small else range(1)

    def ends(t, p):
        return int(direct and t == R - 1 and p >= len(cuts[t]) - straight)

    def row_copy(t, p):
        at = cut(t, p)[0]
        return remote(
            send_buf.at[t, :, at], chunk_buf.at[t, :, at], a_send.at[ends(t, p)], a_recv.at[sem(t, p) - 1], row_of(t), col_me
        )

    def code_copy(t):
        return remote(code_send.at[t], code_recv.at[t], m_send.at[0], m_recv.at[t], row_of(t), col_me)

    def whole(ref, send, recv):
        return remote(ref, ref, send.at[0], recv.at[0], row_of(1), col_me)


    def start_rows(t):
        for p in pieces(t):
            if not ends(t, p):
                row_copy(t, p).start()

    def rows_at(t, block=0, count=None):
        return pl.ds(S + t * CK + block * K, CK if count is None else count)

    def dir_copy(d):
        return remote(
            dir_buf.at[d],
            all_buf.at[rows_at(7, (C - d) % C, K), pl.ds(D - tail, tail)],
            d_send.at[0],
            f_recv.at[sem(7, len(cuts[7]) - straight)],
            row_of(7),
            col_of[d],
        )

    def choose(ts):
        wanted = [one_hot(iota((Q, L), 0) + t * Q == position) for t in ts]
        found = mm(jnp.concatenate(wanted, axis=0), docs_ref[...]).astype(BF16)
        for i, t in enumerate(ts):
            send_buf[t] = found[i * Q : (i + 1) * Q]

    def first_sends():
        pl.semaphore_wait(barrier, R + C - 2)
        each(1, R, lambda t: code_copy(t).start())

    loads[2].wait()
    if R == 8:
        inner = lax.rem(bits[-1] + bits[-2], 2) == 1
        choose([3, 1])
        first_sends()

        @pl.when(inner)
        def _():
            start_rows(3)

        start_rows(1)
        choose([2, 4])
        start_rows(2)
        start_rows(4)

        @pl.when(jnp.logical_not(inner))
        def _():
            start_rows(3)

        choose([5, 6])
        start_rows(5)
        start_rows(6)
        choose([7, 0])
        start_rows(7)
        final = len(cuts[7]) - straight

        @pl.when(inner)
        def _():
            wanted = one_hot(iota((CK, L), 0) == jnp.where(block_i == 7, ahead * K + rank_i, -1))
            found = mm(wanted, docs_ref[:, D - tail :]).astype(BF16)
            dir_buf[...] = found.reshape(dir_buf.shape)

        @pl.when(jnp.logical_not(inner))
        def _():
            for p in range(final, len(cuts[7])):
                row_copy(7, p).start()
    else:
        first_sends()
        group = max(1, R // 2)
        for first in range(0, R, group):
            wanted = one_hot(iota((group * Q, L), 0) + first * Q == position)
            send_buf[first : first + group] = (
                mm(wanted, docs_ref[...]).astype(BF16).reshape(group, Q, D)
            )
            each(max(first, 1), first + group, start_rows)

    def fwd_copy(t, d, p):
        at = cut(t, p)[0]
        return remote(
            fwd_buf.at[t, d - 1, :, at],
            all_buf.at[rows_at(t, C - d, K), at],
            f_send.at[ends(t, p)],
            f_recv.at[sem(t, p)],
            row_me,
            col_of[d],
        )

    def fwd_arrival(t, p):
        ref = all_buf.at[rows_at(t, 1, CK - K), cut(t, p)[0]]
        return remote(ref, ref, f_send.at[0], f_recv.at[sem(t, p)], row_me, col_of[1])

    def tag_copy(t, d):
        return remote(
            tag_send.at[t], tag_recv.at[t, C - d], t_send.at[0], t_recv.at[t], row_me, col_of[d]
        )

    def tag_arrival(t):
        ref = tag_recv.at[t, pl.ds(1, C - 1)]
        return remote(ref, ref, t_send.at[0], t_recv.at[t], row_me, col_of[1])

    block = iota((CK, Q), 0) // K
    turned = jnp.where(block == 0, 0, C - block) * K + iota((CK, Q), 0) - block * K + 1

    def relay(t, p, mine=False):
        if ends(t, p):
            pl.when(jnp.logical_not(inner))(lambda: relay_now(t, p))
        else:
            relay_now(t, p, mine)

    def relay_now(t, p, mine=False):
        if not mine:
            if p == 0 and direct and t == R - 1:
                pl.when(jnp.logical_not(inner))(lambda: code_copy(t).wait_recv())
            elif p == 0:
                code_copy(t).wait_recv()
            row_copy(t, p).wait_recv()
        at, width = cut(t, p)
        lines = (code_send if mine else code_recv)[t][:, :Q]
        line = lines[0:1].astype(jnp.int32)
        wanted = one_hot(iota((CK, Q), 0) + 1 == line)
        if p == 0:
            high = jnp.floor(lines[1:2] * (1.0 / 128.0))
            digits = [high, lines[1:2] - high * 128.0, jnp.zeros((SUB - 2, Q), F32)]
            digits = mm_t(jnp.concatenate(digits, axis=0).astype(BF16), one_hot(turned == line))
            tag_send[t, 0:1, :CK] = 128.0 * digits[0:1] + digits[1:2]
            for d in range(1, C):
                tag_copy(t, d).start()
        found = mm(wanted, (send_buf if mine else chunk_buf)[t, :, at]).astype(BF16)
        fwd_buf[t, :, :, at] = found[K:].reshape(C - 1, K, width)
        for d in range(1, C):
            fwd_copy(t, d, p).start()
        all_buf[rows_at(t, 0, K), at] = found[:K]

    if CK < LANES:
        tag_send[...] = jnp.zeros(tag_send.shape, F32)
    for p in pieces(0):
        relay(0, p, True)

    loads[3].wait()
    norm = jnp.zeros((S, LANES), F32)
    for part in range(0, D, LANES):
        block = all_buf[0:S, part : part + LANES].astype(F32)
        norm = norm + block * block
    cent_mat[...] = jnp.broadcast_to(
        lax.rsqrt(jnp.sum(norm, axis=1, keepdims=True) + 1.0), cent_mat.shape
    )


    eye = iota((CK, CK), 0) == iota((CK, CK), 1)

    def spread(t):
        tag_arrival(t).wait_recv()
        line = tag_send[t][:, :CK]
        for c in range(1, C):
            line = jnp.where(iota((1, CK), 1) // K == c, tag_recv[t, c][:, :CK], line)
        tag_row[t] = line
        tag_mat[t] = jnp.broadcast_to(
            jnp.sum(jnp.where(eye, line, 0.0), axis=1, keepdims=True), (CK, CK)
        )
        best_mat[t] = jnp.zeros((CK, CK), F32)

    stats_ref[...] = jnp.zeros(stats_ref.shape, F32)

    def member_of(t):
        return (iota((S, CK), 0) + 1).astype(F32) == tag_row[t]

    def self_block(t, gram):
        diag = jnp.where(eye, gram, 0.0)
        row_scale = lax.rsqrt(jnp.sum(diag, axis=0, keepdims=True) + 1.0)
        col_scale = lax.rsqrt(jnp.sum(diag, axis=1, keepdims=True) + 1.0)
        inv_row[t] = row_scale
        inv_mat[t] = jnp.broadcast_to(col_scale, (CK, CK))
        line = jnp.where(tag_row[t] > 0.0, tag_row[t], -1.0)
        same = (tag_mat[t] == line) & jnp.logical_not(eye)
        best = jnp.max(jnp.where(same, gram * col_scale, 0.0), axis=0, keepdims=True)
        return row_scale, line, best

    def other_block(u, gram, row_scale, line, best):
        same = tag_mat[u] == line
        best_mat[u] = jnp.maximum(best_mat[u], jnp.where(same, gram * row_scale, 0.0))
        return jnp.maximum(
            best, jnp.max(jnp.where(same, gram * inv_mat[u], 0.0), axis=0, keepdims=True)
        )

    def cross_block(t, cross, row_scale):
        member = member_of(t)
        similarity = row_scale * jnp.sum(
            jnp.where(member, cross * cent_mat[...], 0.0), axis=0, keepdims=True
        )
        sim_row[t] = similarity
        lines = [jnp.ones((1, CK), BF16), *split3(similarity), *split3(similarity * similarity)]
        lines = jnp.concatenate(
            [line.astype(F32) for line in lines] + [jnp.zeros((1, CK), F32)], axis=0
        )
        stats_ref[...] += mm_t(lines.astype(BF16), one_hot(member))

    def settle(t, read):
        row_scale, line, best = self_block(t, read(S + t * CK, CK))
        for u in range(t):
            best = other_block(u, read(S + u * CK, CK), row_scale, line, best)
        best_row[t] = best
        cross_block(t, read(0, S), row_scale)

    def arrivals(t, p):
        fwd_arrival(t, p).wait_recv()

    def absorb_piece(t, p):
        if p == 0:
            spread(t)
        arrivals(t, p)
        at = cut(t, p)[0]
        rows = S + (t + 1) * CK
        before = gram_acc[0:rows] if p else None
        part = mm_t(all_buf[0:rows, at], all_buf[rows_at(t), at])
        gram_acc[0:rows] = part if p == 0 else before + part
        if p == len(cuts[t]) - 1:
            settle(t, lambda start, count: gram_acc[start : start + count])

    def absorb_last():
        t = R - 1
        n = len(cuts[t])
        width = cuts[t][0]
        rows = S + R * CK
        spread(t)

        slow = n - straight - 1

        def step(i, carry):
            p = jnp.where(i < slow, i, jnp.where(i < n - 1, i + 1, slow))
            at = pl.ds(pl.multiple_of(p * width, width), width)
            semaphore = f_recv.at[sem(t, 0) + p]
            @pl.when(jnp.logical_and(inner, p == n - straight))
            def _():
                ref = all_buf.at[rows_at(t), pl.ds(D - tail, tail)]
                remote(ref, ref, d_send.at[0], semaphore, row_me, col_of[1]).wait_recv()

            @pl.when(jnp.logical_or(jnp.logical_not(inner), p < n - straight))
            def _():
                ref = all_buf.at[rows_at(t, 1, CK - K), at]
                remote(ref, ref, d_send.at[0], semaphore, row_me, col_of[1]).wait_recv()

            before = jnp.where(p > 0, gram_acc[0:rows], 0.0)
            gram_acc[0:rows] = before + mm_t(all_buf[0:rows, at], all_buf[rows_at(t), at])
            return carry

        lax.fori_loop(0, n, step, 0)
        settle(t, lambda start, count: gram_acc[start : start + count])

    def absorb(t):
        for p in pieces(t):
            absorb_piece(t, p)

    def absorb_any(t):
        spread(t)
        arrivals(t, 0)
        mine = all_buf[rows_at(t), :]
        row_scale, line, best = self_block(t, mm_t(mine, mine))

        def pair(u, best):
            return other_block(u, mm_t(all_buf[rows_at(u), :], mine), row_scale, line, best)

        best_row[t] = lax.fori_loop(0, t, pair, best)
        cross_block(t, mm_t(all_buf[0:S, :], mine), row_scale)

    def relay_all(*ts):
        for p in pieces(ts[0]):
            for t in ts:
                relay(t, p)

    if R == 8:
        relay_all(1)

        @pl.when(inner)
        def _():
            code_copy(7).wait_recv()
            for d in range(C):
                dir_copy(d).start()

        absorb(0)
        relay_all(2, 3)
        absorb(1)
        relay(4, 0)
        relay(5, 0)
        absorb(2)
        relay(4, 1)
        relay(5, 1)
        absorb(3)
        absorb(4)
        absorb(5)
        for step in plan:
            if step < 0:
                absorb_piece(6, -1 - step)
            else:
                relay(6 + step // 100, step % 100)
        for p in range(len(cuts[7]) - straight, len(cuts[7])):
            relay(7, p)
        absorb_last()
    elif small:
        for t in range(1, R):
            relay_all(t)
            absorb(t - 1)
        absorb(R - 1)
    else:

        def advance(t, carry):
            relay_all(t)
            absorb_any(t - 1)
            return carry

        lax.fori_loop(1, R, advance, 0)
        absorb_any(R - 1)

    stats = stats_ref[...]
    count = stats[0:1]
    total = stats[1:2] + stats[2:3] + stats[3:4]
    square = stats[4:5] + stats[5:6] + stats[6:7]
    floor = jnp.maximum(count, 1.0)
    mean = total / floor
    variance = jnp.maximum(square / floor - mean * mean, 0.0)
    spread_inv = 1.0 / jnp.sqrt(variance + 1.0 / D)
    wanted = [line.astype(F32) for line in (*split3(mean), *split3(spread_inv))]
    wanted = jnp.concatenate(wanted + [jnp.zeros((2, S), F32)], axis=0).astype(BF16)

    def res_copy(t, r, d):
        return remote(
            res_send.at[t], res_recv.at[t * C + (C - d) % C], r_send.at[0], r_recv.at[0], r, col_of[d]
        )

    res_all = whole(res_recv.at[pl.ds(1, O - 1)], r_send, r_recv)

    def finish(t, found):
        centre = found[0:1] + found[1:2] + found[2:3]
        width = found[3:4] + found[4:5] + found[5:6]
        proto = (centre - sim_row[t]) * width
        column = jnp.max(best_mat[t], axis=1, keepdims=True)
        flat = jnp.max(jnp.where(eye, column, 0.0), axis=0, keepdims=True)
        redundant = jnp.maximum(flat, best_row[t]) * inv_row[t] * math.sqrt(D)
        res_send[t, 0:1, :CK] = proto
        res_send[t, 1:2, :CK] = redundant

    if CK < LANES:
        res_send[...] = jnp.zeros(res_send.shape, F32)

    def deliver(t):
        r = row_of(t)
        for d in (2, 3, 1, 0) if C == 4 else range(C):
            if not (isinstance(t, int) and t == 0 and d == 0):
                res_copy(t, r, d).start()

    if small:
        members = jnp.concatenate([one_hot(member_of(t)) for t in range(R)], axis=1)
        found = mm(wanted, members)
        for t in range(R):
            finish(t, found[:, t * CK : (t + 1) * CK])
        for t in [5, 3, 7, 6, 4, 2, 1, 0] if R == 8 else range(R):
            deliver(t)
    else:

        def finish_any(t):
            finish(t, mm(wanted, one_hot(member_of(t))))

        each(0, R, finish_any)
        each(1, R, deliver)
        deliver(0)
    res_recv[0] = res_send[0]
    out_ref[2:3, :S] = count
    out_ref[3:4, :S] = total
    out_ref[4:5, :S] = square

    def sent(ref, semaphore):
        remote(ref, ref, semaphore, r_recv.at[0], row_me, col_of[1]).wait_send()

    if direct:
        kept = D - tail
        sent(send_buf.at[pl.ds(1, R - 2)], a_send.at[0])
        sent(send_buf.at[R - 1, :, pl.ds(0, kept)], a_send.at[0])
        sent(fwd_buf.at[pl.ds(0, R - 1)], f_send.at[0])
        sent(fwd_buf.at[R - 1, :, :, pl.ds(0, kept)], f_send.at[0])

        @pl.when(inner)
        def _():
            sent(dir_buf, d_send.at[0])

        @pl.when(jnp.logical_not(inner))
        def _():
            sent(send_buf.at[R - 1, :, pl.ds(kept, D - kept)], a_send.at[1])
            sent(fwd_buf.at[R - 1, :, :, pl.ds(kept, D - kept)], f_send.at[1])

    else:
        sent(send_buf.at[pl.ds(1, R - 1)], a_send.at[0])
        sent(fwd_buf, f_send.at[0])
    sent(code_recv.at[pl.ds(1, R - 1)], m_send.at[0])
    sent(tag_recv.at[:, pl.ds(1, C - 1)], t_send.at[0])
    res_all.wait_send()
    res_all.wait_recv()

    for o in range(O):
        pair = res_recv[o]
        res_rows[o : o + 1, :] = pair[0:1]
        res_rows[O + o : O + o + 1, :] = pair[1:2]
    parts = jnp.concatenate([line.astype(F32) for line in split3(res_rows[...])], axis=0)
    found = mm(parts.astype(BF16), is_lane)
    found = found[: 2 * O] + found[2 * O : 4 * O] + found[4 * O :]
    mask = iota((O, L), 0) == block_i * C + ahead
    out_ref[0:1, :L] = jnp.sum(jnp.where(mask, found[:O], 0.0), axis=0, keepdims=True)
    out_ref[1:2, :L] = jnp.sum(jnp.where(mask, found[O:], 0.0), axis=0, keepdims=True)


def local(documents, assigned, centroids, owner_slot):
    L, D = documents.shape
    S = centroids.shape[0]
    R = lax.axis_size("dp")
    C = lax.axis_size("cent")
    O = R * C
    pair_cap = 2 * L // O
    row_cap = 5 * C * pair_cap // 8
    K = round_up(pair_cap, 16)
    Q = round_up(row_cap, 16)
    CK = C * K
    QP = round_up(Q, LANES)
    half, unit = D // 2, D // 8
    cuts = [(D,)] + [(half, half)] * (R - 3) + [(2 * unit,) * 4, (unit,) * 8]
    straight = 3
    copies = sum(len(c) for c in cuts) if R <= 8 else R
    T = owner_slot.shape[0] // LANES
    hbm = pl.BlockSpec(memory_space=pl.ANY)
    dma = pltpu.SemaphoreType.DMA
    packed = pl.pallas_call(
        functools.partial(kernel, (R, C, K, Q, cuts, straight)),
        name="cluster_exchange",
        out_shape=pltpu.VMEM((SUB, max(L, S)), F32),
        in_specs=[hbm] * 4,
        out_specs=pl.BlockSpec(memory_space=pltpu.VMEM),
        scratch_shapes=[
            pltpu.VMEM((L, D), BF16),
            pltpu.VMEM((1, L), jnp.int32),
            pltpu.VMEM((T, LANES), jnp.int32),
            pltpu.VMEM((S + R * CK, D), BF16),
            pltpu.VMEM((R, Q, D), BF16),
            pltpu.VMEM((R, Q, D), BF16),
            pltpu.VMEM((R, 2, QP), F32),
            pltpu.VMEM((R, 2, QP), F32),
            pltpu.VMEM((R, C - 1, K, D), BF16),
            pltpu.VMEM((C, K, straight * cuts[-1][-1]), BF16),
            pltpu.VMEM((R, 1, LANES), F32),
            pltpu.VMEM((R, C, 1, LANES), F32),
            pltpu.VMEM((R, 2, LANES), F32),
            pltpu.VMEM((O, 2, LANES), F32),
            pltpu.VMEM((2 * O, LANES), F32),
            pltpu.VMEM((R, 1, CK), F32),
            pltpu.VMEM((R, CK, CK), F32),
            pltpu.VMEM((R, 1, CK), F32),
            pltpu.VMEM((R, CK, CK), F32),
            pltpu.VMEM((R, 1, CK), F32),
            pltpu.VMEM((R, 1, CK), F32),
            pltpu.VMEM((R, CK, CK), F32),
            pltpu.VMEM((S, CK), F32),
            pltpu.VMEM((S + R * CK if R <= 8 else SUB, CK), F32),
            pltpu.VMEM((SUB, S), F32),
            dma((4,)),
            dma((2,)),
            dma((copies - 1,)),
            dma((1,)),
            dma((R,)),
            dma((2,)),
            dma((copies,)),
            dma((1,)),
            dma((R,)),
            dma((1,)),
            dma((1,)),
            dma((1,)),
        ],
        compiler_params=pltpu.CompilerParams(
            collective_id=0, has_side_effects=True, vmem_limit_bytes=62 * 1024 * 1024
        ),
    )(
        documents,
        assigned.reshape(1, L),
        centroids,
        owner_slot.reshape(-1, LANES),
    )

    def spill(packed_ref, proto_ref, red_ref, stats_ref, sems):
        copies = [
            pltpu.make_async_copy(packed_ref.at[pl.ds(0, 1), pl.ds(0, L)], proto_ref, sems.at[0]),
            pltpu.make_async_copy(packed_ref.at[pl.ds(1, 1), pl.ds(0, L)], red_ref, sems.at[1]),
            pltpu.make_async_copy(packed_ref.at[pl.ds(2, 3), pl.ds(0, S)], stats_ref, sems.at[2]),
        ]
        for copy in copies:
            copy.start()
        for copy in copies:
            copy.wait()

    proto, red, stats = pl.pallas_call(
        spill,
        name="spill",
        out_shape=[jax.ShapeDtypeStruct((1, L), F32)] * 2 + [jax.ShapeDtypeStruct((3, S), F32)],
        in_specs=[pl.BlockSpec(memory_space=pltpu.VMEM)],
        out_specs=[hbm] * 3,
        scratch_shapes=[dma((3,))],
    )(pltpu.with_memory_space_constraint(packed, pltpu.VMEM))
    return proto.reshape(L), red.reshape(L), stats


def solution(mesh):
    in_specs = (P(("dp", "cent"), None), P(("dp", "cent")), P(("dp", "cent"), None), P())
    out_specs = (P(("dp", "cent")), P(("dp", "cent")), P(None, ("dp", "cent")))
    return jax.shard_map(local, mesh=mesh, in_specs=in_specs, out_specs=out_specs, check_vma=False)
```

```python
import functools
import math

import jax
import jax.numpy as jnp
from jax import lax
from jax.experimental import pallas as pl
from jax.experimental.pallas import tpu as pltpu
from jax.sharding import PartitionSpec as P

F32 = jnp.float32
BF16 = jnp.bfloat16
LANES = 128
SUB = 8


def round_up(value, unit):
    return -(-value // unit) * unit


def each(low, high, body):
    if high - low <= 8:
        for step in range(low, high):
            body(step)
    else:
        lax.fori_loop(low, high, lambda step, carry: (body(step), carry)[1], 0)


def iota(shape, dim):
    return lax.broadcasted_iota(jnp.int32, shape, dim)


def mm(left, right):
    return lax.dot_general(left, right, (((1,), (0,)), ((), ())), preferred_element_type=F32)


def mm_t(left, right):
    return lax.dot_general(left, right, (((1,), (1,)), ((), ())), preferred_element_type=F32)


def one_hot(condition):
    return jnp.where(condition, 1.0, 0.0).astype(BF16)


def split3(value):
    high = value.astype(BF16)
    rest = value - high.astype(F32)
    mid = rest.astype(BF16)
    low = (rest - mid.astype(F32)).astype(BF16)
    return high, mid, low


def kernel(
    dims,
    docs_hbm,
    assigned_hbm,
    cent_hbm,
    table_hbm,
    out_ref,
    docs_ref,
    assigned_ref,
    table_ref,
    all_buf,
    send_buf,
    chunk_buf,
    code_send,
    code_recv,
    fwd_buf,
    dir_buf,
    tag_send,
    tag_recv,
    res_send,
    res_recv,
    res_rows,
    tag_row,
    tag_mat,
    inv_row,
    inv_mat,
    sim_row,
    best_row,
    best_mat,
    cent_mat,
    gram_acc,
    stats_ref,
    in_sem,
    a_send,
    a_recv,
    m_send,
    m_recv,
    f_send,
    f_recv,
    t_send,
    t_recv,
    r_send,
    r_recv,
    d_send,
):
    R, C, K, Q, cuts, straight = dims
    tail = straight * cuts[-1][-1]
    O = R * C
    CK = C * K
    L, D = docs_ref.shape
    S = cent_hbm.shape[0]
    T = table_ref.shape[0]
    QP = code_send.shape[2]
    small = R <= 8
    direct = R == 8
    row_me = lax.axis_index("dp")
    col_me = lax.axis_index("cent")
    own = row_me * C + col_me

    bits = []
    while 2 ** len(bits) < R:
        bits.append(lax.rem(lax.div(row_me, 2 ** len(bits)), 2))
    col_of = [col_me] + [lax.rem(col_me + d, C) for d in range(1, C)]

    swap = {3: 4, 4: 3} if R == 8 else {}

    def row_of(t):
        total = 0
        if isinstance(t, int):
            t = swap.get(t, t)
        for i, bit in enumerate(bits):
            if isinstance(t, int):
                total = total + (1 - bit if (t >> i) & 1 else bit) * 2**i
            else:
                total = total + lax.rem(bit + lax.div(t, 2**i), 2) * 2**i
        return total

    def all_peers(body):
        def at_row(t):
            r = row_of(t)
            for d in range(C):
                body(t, r, d)

        each(1, R, at_row)
        for d in range(1, C):
            body(0, row_me, d)

    def where_is(r, c):
        return {"dp": r, "cent": c}

    def remote(src, dst, send, recv, r, c):
        return pltpu.make_async_remote_copy(
            src_ref=src,
            dst_ref=dst,
            send_sem=send,
            recv_sem=recv,
            device_id=where_is(r, c),
            device_id_type=pl.DeviceIdType.MESH,
        )

    barrier = pltpu.get_barrier_semaphore()

    def greet(r, c):
        pl.semaphore_signal(
            barrier, inc=1, device_id=where_is(r, c), device_id_type=pl.DeviceIdType.MESH
        )

    each(1, R, lambda t: greet(row_of(t), col_me))
    for d in range(1, C):
        greet(row_me, col_of[d])

    cent_rows = all_buf.at[pl.ds(0, S), :]
    loads = [
        pltpu.make_async_copy(assigned_hbm, assigned_ref, in_sem.at[0]),
        pltpu.make_async_copy(table_hbm, table_ref, in_sem.at[1]),
        pltpu.make_async_copy(docs_hbm, docs_ref, in_sem.at[2]),
        pltpu.make_async_copy(cent_hbm, cent_rows, in_sem.at[3]),
    ]
    for load in loads:
        load.start()
    loads[0].wait()
    loads[1].wait()

    assigned = assigned_ref[...]
    high = lax.shift_right_logical(assigned, 7)
    low = jnp.bitwise_and(assigned, 127)
    table = table_ref[...]
    pick = one_hot(iota((T, L), 0) == high)
    looked = jnp.zeros((LANES, L), F32)
    shift = 0
    while 2**shift < O * S:
        digit = jnp.bitwise_and(lax.shift_right_logical(table, shift), 255)
        looked = looked + float(2**shift) * lax.dot_general(
            digit.astype(F32).astype(BF16), pick, (((0,), (0,)), ((), ())), preferred_element_type=F32
        )
        shift += 8
    slot = jnp.sum(jnp.where(iota((LANES, L), 0) == low, looked, 0.0), axis=0, keepdims=True)
    owner = jnp.floor((slot + 0.5) * (1.0 / S))
    row = jnp.floor((owner + 0.5) * (1.0 / C))
    owner_i = owner.astype(jnp.int32)
    row_i = row.astype(jnp.int32)
    cent_i = owner_i - row_i * C
    is_owner = jnp.where(iota((O, L), 0) == owner_i, 1.0, 0.0)
    is_row = jnp.where(iota((R, L), 0) == row_i, 1.0, 0.0)
    earlier = one_hot(iota((L, L), 0) < iota((L, L), 1))
    ranks = mm(jnp.concatenate([is_owner, is_row], axis=0).astype(BF16), earlier)
    rank_owner = jnp.sum(ranks[:O] * is_owner, axis=0, keepdims=True)
    rank_row = jnp.sum(ranks[O:] * is_row, axis=0, keepdims=True)
    block_i = jnp.bitwise_xor(row_i, row_me)
    if swap:
        block_i = jnp.where((block_i == 3) | (block_i == 4), 7 - block_i, block_i)
    position = block_i * Q + rank_row.astype(jnp.int32)
    rank_i = rank_owner.astype(jnp.int32)

    ahead = cent_i - col_me
    ahead = jnp.where(ahead < 0, ahead + C, ahead)
    behind = jnp.where(ahead == 0, 0, C - ahead)
    lane_i = behind * K + rank_i
    is_lane = one_hot(iota((LANES, L), 0) == lane_i)

    tag = slot - owner * S + 1.0
    tag_hi = jnp.floor(tag * (1.0 / 128.0))
    lines = jnp.concatenate(
        [(ahead * K + rank_i + 1).astype(F32), tag_hi, tag - tag_hi * 128.0, jnp.zeros((SUB - 3, L), F32)],
        axis=0,
    ).astype(BF16)

    def mark(t):
        here = jnp.where(position < (t + 1) * Q, position, -1)
        line = mm_t(lines, one_hot(iota((QP, L), 0) + t * Q == here))
        code_send[t, 0:1, :] = line[0:1]
        code_send[t, 1:2, :] = 128.0 * line[1:2] + line[2:3]

    each(0, R, mark)

    def cut(t, p):
        width = cuts[t][p] if small else D
        return pl.ds(sum(cuts[t][:p]) if small else 0, width), width

    def sem(t, p):
        return sum(len(c) for c in cuts[:t]) + p if small else t

    def pieces(t):
        return range(len(cuts[t])) if small else range(1)

    def ends(t, p):
        return int(direct and t == R - 1 and p >= len(cuts[t]) - straight)

    def row_copy(t, p):
        at = cut(t, p)[0]
        return remote(
            send_buf.at[t, :, at], chunk_buf.at[t, :, at], a_send.at[ends(t, p)], a_recv.at[sem(t, p) - 1], row_of(t), col_me
        )

    def code_group(t):
        return (0 if t == 1 else 2 if t == R - 1 else 1) if direct else t

    def code_copy(t):
        return remote(code_send.at[t], code_recv.at[t], m_send.at[0], m_recv.at[code_group(t)], row_of(t), col_me)

    def whole(ref, send, recv):
        return remote(ref, ref, send.at[0], recv.at[0], row_of(1), col_me)


    def start_rows(t):
        for p in pieces(t):
            if not ends(t, p):
                row_copy(t, p).start()

    def rows_at(t, block=0, count=None):
        return pl.ds(S + t * CK + block * K, CK if count is None else count)

    def dir_copy(d, p):
        at, width = cut(7, p)
        return remote(
            dir_buf.at[d, :, pl.ds((p - len(cuts[7]) + straight) * width, width)],
            all_buf.at[rows_at(7, (C - d) % C, K), at],
            d_send.at[0],
            f_recv.at[sem(7, p)],
            row_of(7),
            col_of[d],
        )

    def choose(ts):
        wanted = [one_hot(iota((Q, L), 0) + t * Q == position) for t in ts]
        found = mm(jnp.concatenate(wanted, axis=0), docs_ref[...]).astype(BF16)
        for i, t in enumerate(ts):
            send_buf[t] = found[i * Q : (i + 1) * Q]

    def first_sends():
        pl.semaphore_wait(barrier, R + C - 2)
        each(1, R, lambda t: code_copy(t).start())

    loads[2].wait()
    if R == 8:
        inner = lax.rem(bits[-1] + bits[-2], 2) == 1
        choose([3, 1])
        first_sends()

        @pl.when(inner)
        def _():
            start_rows(3)

        start_rows(1)
        choose([2, 4])
        start_rows(2)
        start_rows(4)

        @pl.when(jnp.logical_not(inner))
        def _():
            start_rows(3)

        choose([5, 6])
        start_rows(5)
        start_rows(6)
        choose([7, 0])
        start_rows(7)
        final = len(cuts[7]) - straight

        @pl.when(inner)
        def _():
            wanted = one_hot(iota((CK, L), 0) == jnp.where(block_i == 7, ahead * K + rank_i, -1))
            found = mm(wanted, docs_ref[:, D - tail :]).astype(BF16)
            dir_buf[...] = found.reshape(dir_buf.shape)

        @pl.when(jnp.logical_not(inner))
        def _():
            for p in range(final, len(cuts[7])):
                row_copy(7, p).start()
    else:
        first_sends()
        group = max(1, R // 2)
        for first in range(0, R, group):
            wanted = one_hot(iota((group * Q, L), 0) + first * Q == position)
            send_buf[first : first + group] = (
                mm(wanted, docs_ref[...]).astype(BF16).reshape(group, Q, D)
            )
            each(max(first, 1), first + group, start_rows)

    def fwd_copy(t, d, p):
        at = cut(t, p)[0]
        return remote(
            fwd_buf.at[t, d - 1, :, at],
            all_buf.at[rows_at(t, C - d, K), at],
            f_send.at[ends(t, p)],
            f_recv.at[sem(t, p)],
            row_me,
            col_of[d],
        )

    def fwd_arrival(t, p):
        ref = all_buf.at[rows_at(t, 1, CK - K), cut(t, p)[0]]
        return remote(ref, ref, f_send.at[0], f_recv.at[sem(t, p)], row_me, col_of[1])

    def tag_copy(t, d):
        return remote(
            tag_send.at[t], tag_recv.at[t, C - d], t_send.at[0], t_recv.at[t], row_me, col_of[d]
        )

    def tag_arrival(t):
        ref = tag_recv.at[t, pl.ds(1, C - 1)]
        return remote(ref, ref, t_send.at[0], t_recv.at[t], row_me, col_of[1])

    block = iota((CK, Q), 0) // K
    turned = jnp.where(block == 0, 0, C - block) * K + iota((CK, Q), 0) - block * K + 1

    def relay(t, p, mine=False):
        if ends(t, p):
            pl.when(jnp.logical_not(inner))(lambda: relay_now(t, p))
        else:
            relay_now(t, p, mine)

    def relay_now(t, p, mine=False):
        if not mine:
            if p == 0 and direct and t == R - 1:
                pl.when(jnp.logical_not(inner))(lambda: code_copy(t).wait_recv())
            elif p == 0 and not (direct and 1 < t < R - 1):
                code_copy(t).wait_recv()
            row_copy(t, p).wait_recv()
        at, width = cut(t, p)
        lines = (code_send if mine else code_recv)[t][:, :Q]
        line = lines[0:1].astype(jnp.int32)
        wanted = one_hot(iota((CK, Q), 0) + 1 == line)
        if p == 0:
            high = jnp.floor(lines[1:2] * (1.0 / 128.0))
            digits = [high, lines[1:2] - high * 128.0, jnp.zeros((SUB - 2, Q), F32)]
            digits = mm_t(jnp.concatenate(digits, axis=0).astype(BF16), one_hot(turned == line))
            tag_send[t, 0:1, :CK] = 128.0 * digits[0:1] + digits[1:2]
            for d in range(1, C):
                tag_copy(t, d).start()
        found = mm(wanted, (send_buf if mine else chunk_buf)[t, :, at]).astype(BF16)
        fwd_buf[t, :, :, at] = found[K:].reshape(C - 1, K, width)
        for d in range(1, C):
            fwd_copy(t, d, p).start()
        all_buf[rows_at(t, 0, K), at] = found[:K]

    if CK < LANES:
        tag_send[...] = jnp.zeros(tag_send.shape, F32)
    for p in pieces(0):
        relay(0, p, True)

    loads[3].wait()
    norm = jnp.zeros((S, LANES), F32)
    for part in range(0, D, LANES):
        block = all_buf[0:S, part : part + LANES].astype(F32)
        norm = norm + block * block
    cent_mat[...] = jnp.broadcast_to(
        lax.rsqrt(jnp.sum(norm, axis=1, keepdims=True) + 1.0), cent_mat.shape
    )


    eye = iota((CK, CK), 0) == iota((CK, CK), 1)

    def spread(t):
        tag_arrival(t).wait_recv()
        line = tag_send[t][:, :CK]
        for c in range(1, C):
            line = jnp.where(iota((1, CK), 1) // K == c, tag_recv[t, c][:, :CK], line)
        tag_row[t] = line
        tag_mat[t] = jnp.broadcast_to(
            jnp.sum(jnp.where(eye, line, 0.0), axis=1, keepdims=True), (CK, CK)
        )
        best_mat[t] = jnp.zeros((CK, CK), F32)

    stats_ref[...] = jnp.zeros(stats_ref.shape, F32)

    def member_of(t):
        return (iota((S, CK), 0) + 1).astype(F32) == tag_row[t]

    def self_block(t, gram):
        diag = jnp.where(eye, gram, 0.0)
        row_scale = lax.rsqrt(jnp.sum(diag, axis=0, keepdims=True) + 1.0)
        col_scale = lax.rsqrt(jnp.sum(diag, axis=1, keepdims=True) + 1.0)
        inv_row[t] = row_scale
        inv_mat[t] = jnp.broadcast_to(col_scale, (CK, CK))
        line = jnp.where(tag_row[t] > 0.0, tag_row[t], -1.0)
        same = (tag_mat[t] == line) & jnp.logical_not(eye)
        best = jnp.max(jnp.where(same, gram * col_scale, 0.0), axis=0, keepdims=True)
        return row_scale, line, best

    def other_block(u, gram, row_scale, line, best):
        same = tag_mat[u] == line
        best_mat[u] = jnp.maximum(best_mat[u], jnp.where(same, gram * row_scale, 0.0))
        return jnp.maximum(
            best, jnp.max(jnp.where(same, gram * inv_mat[u], 0.0), axis=0, keepdims=True)
        )

    def cross_block(t, cross, row_scale):
        member = member_of(t)
        similarity = row_scale * jnp.sum(
            jnp.where(member, cross * cent_mat[...], 0.0), axis=0, keepdims=True
        )
        sim_row[t] = similarity
        lines = [jnp.ones((1, CK), BF16), *split3(similarity), *split3(similarity * similarity)]
        lines = jnp.concatenate(
            [line.astype(F32) for line in lines] + [jnp.zeros((1, CK), F32)], axis=0
        )
        stats_ref[...] += mm_t(lines.astype(BF16), one_hot(member))

    def settle(t, read):
        row_scale, line, best = self_block(t, read(S + t * CK, CK))
        for u in range(t):
            best = other_block(u, read(S + u * CK, CK), row_scale, line, best)
        best_row[t] = best
        cross_block(t, read(0, S), row_scale)

    def arrivals(t, p):
        fwd_arrival(t, p).wait_recv()

    def absorb_piece(t, p):
        if p == 0:
            spread(t)
        arrivals(t, p)
        at = cut(t, p)[0]
        rows = S + (t + 1) * CK
        before = gram_acc[0:rows] if p else None
        part = mm_t(all_buf[0:rows, at], all_buf[rows_at(t), at])
        gram_acc[0:rows] = part if p == 0 else before + part
        if p == len(cuts[t]) - 1:
            settle(t, lambda start, count: gram_acc[start : start + count])

    def absorb_loop(t):
        n = len(cuts[t])
        width = cuts[t][0]
        rows = S + (t + 1) * CK
        first_straight = n - straight if t == R - 1 else n
        slow = first_straight - 1
        spread(t)

        def step(i, carry):
            p = i
            if first_straight < n:
                ahead_of = jnp.logical_and(i >= slow, i < n - 2)
                p = jnp.where(i == n - 2, slow, i + jnp.where(ahead_of, 1, 0))
            at = pl.ds(pl.multiple_of(p * width, width), width)
            semaphore = f_recv.at[sem(t, 0) + p]

            def relayed():
                ref = all_buf.at[rows_at(t, 1, CK - K), at]
                remote(ref, ref, d_send.at[0], semaphore, row_me, col_of[1]).wait_recv()

            if first_straight < n:

                @pl.when(jnp.logical_and(inner, p >= first_straight))
                def _():
                    ref = all_buf.at[rows_at(t), at]
                    remote(ref, ref, d_send.at[0], semaphore, row_me, col_of[1]).wait_recv()

                pl.when(jnp.logical_or(jnp.logical_not(inner), p < first_straight))(relayed)
            else:
                relayed()
            before = jnp.where(i > 0, gram_acc[0:rows], 0.0)
            gram_acc[0:rows] = before + mm_t(all_buf[0:rows, at], all_buf[rows_at(t), at])
            return carry

        lax.fori_loop(0, n, step, 0)
        settle(t, lambda start, count: gram_acc[start : start + count])

    def absorb(t):
        for p in pieces(t):
            absorb_piece(t, p)

    def absorb_any(t):
        spread(t)
        arrivals(t, 0)
        mine = all_buf[rows_at(t), :]
        row_scale, line, best = self_block(t, mm_t(mine, mine))

        def pair(u, best):
            return other_block(u, mm_t(all_buf[rows_at(u), :], mine), row_scale, line, best)

        best_row[t] = lax.fori_loop(0, t, pair, best)
        cross_block(t, mm_t(all_buf[0:S, :], mine), row_scale)

    def relay_all(*ts):
        for p in pieces(ts[0]):
            for t in ts:
                relay(t, p)

    if R == 8:
        relay_all(1)

        @pl.when(inner)
        def _():
            code_copy(7).wait_recv()
            for p in range(len(cuts[7]) - straight, len(cuts[7])):
                for d in range(C):
                    dir_copy(d, p).start()

        absorb(0)
        ref = code_recv.at[pl.ds(2, R - 3)]
        remote(ref, ref, m_send.at[0], m_recv.at[1], row_of(1), col_me).wait_recv()

        @pl.when(inner)
        def _():
            relay_all(2, 3)

        @pl.when(jnp.logical_not(inner))
        def _():
            relay_all(3, 2)

        absorb(1)
        relay(4, 0)
        relay(5, 0)
        absorb(2)
        relay(4, 1)
        relay(5, 1)
        absorb(3)
        absorb(4)
        absorb(5)
        relay_all(6)
        relay_all(7)
        absorb_loop(6)
        absorb_loop(R - 1)
    elif small:
        for t in range(1, R):
            relay_all(t)
            absorb(t - 1)
        absorb(R - 1)
    else:

        def advance(t, carry):
            relay_all(t)
            absorb_any(t - 1)
            return carry

        lax.fori_loop(1, R, advance, 0)
        absorb_any(R - 1)

    stats = stats_ref[...]
    count = stats[0:1]
    total = stats[1:2] + stats[2:3] + stats[3:4]
    square = stats[4:5] + stats[5:6] + stats[6:7]
    share = 1.0 / jnp.maximum(count, 1.0)
    mean = total * share
    variance = jnp.maximum(square * share - mean * mean, 0.0)
    spread_inv = lax.rsqrt(variance + 1.0 / D)
    wanted = [line.astype(F32) for line in (*split3(mean), *split3(spread_inv))]
    wanted = jnp.concatenate(wanted + [jnp.zeros((2, S), F32)], axis=0).astype(BF16)

    def res_copy(t, r, d):
        return remote(
            res_send.at[t], res_recv.at[t * C + (C - d) % C], r_send.at[0], r_recv.at[0], r, col_of[d]
        )

    res_all = whole(res_recv.at[pl.ds(1, O - 1)], r_send, r_recv)

    def finish(t, found):
        centre = found[0:1] + found[1:2] + found[2:3]
        width = found[3:4] + found[4:5] + found[5:6]
        proto = (centre - sim_row[t]) * width
        column = jnp.max(best_mat[t], axis=1, keepdims=True)
        flat = jnp.max(jnp.where(eye, column, 0.0), axis=0, keepdims=True)
        redundant = jnp.maximum(flat, best_row[t]) * inv_row[t] * math.sqrt(D)
        res_send[t, 0:1, :CK] = proto
        res_send[t, 1:2, :CK] = redundant

    if CK < LANES:
        res_send[...] = jnp.zeros(res_send.shape, F32)

    def deliver(t):
        r = row_of(t)
        for d in (2, 3, 1, 0) if C == 4 else range(C):
            if not (isinstance(t, int) and t == 0 and d == 0):
                res_copy(t, r, d).start()

    if small:
        members = jnp.concatenate([one_hot(member_of(t)) for t in range(R)], axis=1)
        found = mm(wanted, members)
        for t in range(R):
            finish(t, found[:, t * CK : (t + 1) * CK])
        for t in [5, 3, 7, 6, 4, 2, 1, 0] if R == 8 else range(R):
            deliver(t)
    else:

        def finish_any(t):
            finish(t, mm(wanted, one_hot(member_of(t))))

        each(0, R, finish_any)
        each(1, R, deliver)
        deliver(0)
    res_recv[0] = res_send[0]
    out_ref[2:3, :S] = count
    out_ref[3:4, :S] = total
    out_ref[4:5, :S] = square

    def sent(ref, semaphore):
        remote(ref, ref, semaphore, r_recv.at[0], row_me, col_of[1]).wait_send()

    if direct:
        kept = D - tail
        sent(send_buf.at[pl.ds(1, R - 2)], a_send.at[0])
        sent(send_buf.at[R - 1, :, pl.ds(0, kept)], a_send.at[0])
        sent(fwd_buf.at[pl.ds(0, R - 1)], f_send.at[0])
        sent(fwd_buf.at[R - 1, :, :, pl.ds(0, kept)], f_send.at[0])

        @pl.when(inner)
        def _():
            sent(dir_buf, d_send.at[0])

        @pl.when(jnp.logical_not(inner))
        def _():
            sent(send_buf.at[R - 1, :, pl.ds(kept, D - kept)], a_send.at[1])
            sent(fwd_buf.at[R - 1, :, :, pl.ds(kept, D - kept)], f_send.at[1])

    else:
        sent(send_buf.at[pl.ds(1, R - 1)], a_send.at[0])
        sent(fwd_buf, f_send.at[0])
    sent(code_recv.at[pl.ds(1, R - 1)], m_send.at[0])
    sent(tag_recv.at[:, pl.ds(1, C - 1)], t_send.at[0])
    res_all.wait_send()
    res_all.wait_recv()

    for o in range(O):
        pair = res_recv[o]
        res_rows[o : o + 1, :] = pair[0:1]
        res_rows[O + o : O + o + 1, :] = pair[1:2]
    parts = jnp.concatenate([line.astype(F32) for line in split3(res_rows[...])], axis=0)
    found = mm(parts.astype(BF16), is_lane)
    found = found[: 2 * O] + found[2 * O : 4 * O] + found[4 * O :]
    mask = iota((O, L), 0) == block_i * C + ahead
    out_ref[0:1, :L] = jnp.sum(jnp.where(mask, found[:O], 0.0), axis=0, keepdims=True)
    out_ref[1:2, :L] = jnp.sum(jnp.where(mask, found[O:], 0.0), axis=0, keepdims=True)


def local(documents, assigned, centroids, owner_slot):
    L, D = documents.shape
    S = centroids.shape[0]
    R = lax.axis_size("dp")
    C = lax.axis_size("cent")
    O = R * C
    pair_cap = 2 * L // O
    row_cap = 5 * C * pair_cap // 8
    K = round_up(pair_cap, 16)
    Q = round_up(row_cap, 16)
    CK = C * K
    QP = round_up(Q, LANES)
    half, unit = D // 2, D // 8
    cuts = [(D,)] + [(half, half)] * (R - 3) + [(2 * unit,) * 4, (2 * unit,) * 4]
    straight = 2
    copies = sum(len(c) for c in cuts) if R <= 8 else R
    T = owner_slot.shape[0] // LANES
    hbm = pl.BlockSpec(memory_space=pl.ANY)
    dma = pltpu.SemaphoreType.DMA
    packed = pl.pallas_call(
        functools.partial(kernel, (R, C, K, Q, cuts, straight)),
        name="cluster_exchange",
        out_shape=pltpu.VMEM((SUB, max(L, S)), F32),
        in_specs=[hbm] * 4,
        out_specs=pl.BlockSpec(memory_space=pltpu.VMEM),
        scratch_shapes=[
            pltpu.VMEM((L, D), BF16),
            pltpu.VMEM((1, L), jnp.int32),
            pltpu.VMEM((T, LANES), jnp.int32),
            pltpu.VMEM((S + R * CK, D), BF16),
            pltpu.VMEM((R, Q, D), BF16),
            pltpu.VMEM((R, Q, D), BF16),
            pltpu.VMEM((R, 2, QP), F32),
            pltpu.VMEM((R, 2, QP), F32),
            pltpu.VMEM((R, C - 1, K, D), BF16),
            pltpu.VMEM((C, K, straight * cuts[-1][-1]), BF16),
            pltpu.VMEM((R, 1, LANES), F32),
            pltpu.VMEM((R, C, 1, LANES), F32),
            pltpu.VMEM((R, 2, LANES), F32),
            pltpu.VMEM((O, 2, LANES), F32),
            pltpu.VMEM((2 * O, LANES), F32),
            pltpu.VMEM((R, 1, CK), F32),
            pltpu.VMEM((R, CK, CK), F32),
            pltpu.VMEM((R, 1, CK), F32),
            pltpu.VMEM((R, CK, CK), F32),
            pltpu.VMEM((R, 1, CK), F32),
            pltpu.VMEM((R, 1, CK), F32),
            pltpu.VMEM((R, CK, CK), F32),
            pltpu.VMEM((S, CK), F32),
            pltpu.VMEM((S + R * CK if R <= 8 else SUB, CK), F32),
            pltpu.VMEM((SUB, S), F32),
            dma((4,)),
            dma((2,)),
            dma((copies - 1,)),
            dma((1,)),
            dma((3 if R == 8 else R,)),
            dma((2,)),
            dma((copies,)),
            dma((1,)),
            dma((R,)),
            dma((1,)),
            dma((1,)),
            dma((1,)),
        ],
        compiler_params=pltpu.CompilerParams(
            collective_id=0, has_side_effects=True, vmem_limit_bytes=62 * 1024 * 1024
        ),
    )(
        documents,
        assigned.reshape(1, L),
        centroids,
        owner_slot.reshape(-1, LANES),
    )

    def spill(packed_ref, proto_ref, red_ref, stats_ref, sems):
        copies = [
            pltpu.make_async_copy(packed_ref.at[pl.ds(0, 1), pl.ds(0, L)], proto_ref, sems.at[0]),
            pltpu.make_async_copy(packed_ref.at[pl.ds(1, 1), pl.ds(0, L)], red_ref, sems.at[1]),
            pltpu.make_async_copy(packed_ref.at[pl.ds(2, 3), pl.ds(0, S)], stats_ref, sems.at[2]),
        ]
        for copy in copies:
            copy.start()
        for copy in copies:
            copy.wait()

    proto, red, stats = pl.pallas_call(
        spill,
        name="spill",
        out_shape=[jax.ShapeDtypeStruct((1, L), F32)] * 2 + [jax.ShapeDtypeStruct((3, S), F32)],
        in_specs=[pl.BlockSpec(memory_space=pltpu.VMEM)],
        out_specs=[hbm] * 3,
        scratch_shapes=[dma((3,))],
    )(pltpu.with_memory_space_constraint(packed, pltpu.VMEM))
    return proto.reshape(L), red.reshape(L), stats


def solution(mesh):
    in_specs = (P(("dp", "cent"), None), P(("dp", "cent")), P(("dp", "cent"), None), P())
    out_specs = (P(("dp", "cent")), P(("dp", "cent")), P(None, ("dp", "cent")))
    return jax.shard_map(local, mesh=mesh, in_specs=in_specs, out_specs=out_specs, check_vma=False)
```

```python
import functools
import math

import jax
import jax.numpy as jnp
from jax import lax
from jax.experimental import pallas as pl
from jax.experimental.pallas import tpu as pltpu
from jax.sharding import PartitionSpec as P

F32 = jnp.float32
BF16 = jnp.bfloat16
LANES = 128
SUB = 8


def round_up(value, unit):
    return -(-value // unit) * unit


def each(low, high, body):
    if high - low <= 8:
        for step in range(low, high):
            body(step)
    else:
        lax.fori_loop(low, high, lambda step, carry: (body(step), carry)[1], 0)


def iota(shape, dim):
    return lax.broadcasted_iota(jnp.int32, shape, dim)


def mm(left, right):
    return lax.dot_general(left, right, (((1,), (0,)), ((), ())), preferred_element_type=F32)


def mm_t(left, right):
    return lax.dot_general(left, right, (((1,), (1,)), ((), ())), preferred_element_type=F32)


def one_hot(condition):
    return jnp.where(condition, 1.0, 0.0).astype(BF16)


def split3(value):
    high = value.astype(BF16)
    rest = value - high.astype(F32)
    mid = rest.astype(BF16)
    low = (rest - mid.astype(F32)).astype(BF16)
    return high, mid, low


def kernel(
    dims,
    docs_hbm,
    assigned_hbm,
    cent_hbm,
    table_hbm,
    out_ref,
    docs_ref,
    assigned_ref,
    table_ref,
    all_buf,
    send_buf,
    chunk_buf,
    code_send,
    code_recv,
    fwd_buf,
    dir_buf,
    tag_send,
    tag_recv,
    res_send,
    res_recv,
    res_rows,
    tag_row,
    tag_mat,
    inv_row,
    inv_mat,
    sim_row,
    best_row,
    best_mat,
    cent_mat,
    gram_acc,
    stats_ref,
    in_sem,
    a_send,
    a_recv,
    m_send,
    m_recv,
    f_send,
    f_recv,
    t_send,
    t_recv,
    r_send,
    r_recv,
    d_send,
):
    R, C, K, Q, cuts, straight = dims
    tail = straight * cuts[-1][-1]
    O = R * C
    CK = C * K
    L, D = docs_ref.shape
    S = cent_hbm.shape[0]
    T = table_ref.shape[0]
    QP = code_send.shape[2]
    small = R <= 8
    direct = R == 8
    row_me = lax.axis_index("dp")
    col_me = lax.axis_index("cent")
    own = row_me * C + col_me

    bits = []
    while 2 ** len(bits) < R:
        bits.append(lax.rem(lax.div(row_me, 2 ** len(bits)), 2))
    col_of = [col_me] + [lax.rem(col_me + d, C) for d in range(1, C)]

    swap = {3: 4, 4: 3} if R == 8 else {}

    def row_of(t):
        total = 0
        if isinstance(t, int):
            t = swap.get(t, t)
        for i, bit in enumerate(bits):
            if isinstance(t, int):
                total = total + (1 - bit if (t >> i) & 1 else bit) * 2**i
            else:
                total = total + lax.rem(bit + lax.div(t, 2**i), 2) * 2**i
        return total

    def all_peers(body):
        def at_row(t):
            r = row_of(t)
            for d in range(C):
                body(t, r, d)

        each(1, R, at_row)
        for d in range(1, C):
            body(0, row_me, d)

    def where_is(r, c):
        return {"dp": r, "cent": c}

    def remote(src, dst, send, recv, r, c):
        return pltpu.make_async_remote_copy(
            src_ref=src,
            dst_ref=dst,
            send_sem=send,
            recv_sem=recv,
            device_id=where_is(r, c),
            device_id_type=pl.DeviceIdType.MESH,
        )

    barrier = pltpu.get_barrier_semaphore()

    def greet(r, c):
        pl.semaphore_signal(
            barrier, inc=1, device_id=where_is(r, c), device_id_type=pl.DeviceIdType.MESH
        )

    each(1, R, lambda t: greet(row_of(t), col_me))
    for d in range(1, C):
        greet(row_me, col_of[d])

    cent_rows = all_buf.at[pl.ds(0, S), :]
    loads = [
        pltpu.make_async_copy(assigned_hbm, assigned_ref, in_sem.at[0]),
        pltpu.make_async_copy(table_hbm, table_ref, in_sem.at[1]),
        pltpu.make_async_copy(docs_hbm, docs_ref, in_sem.at[2]),
        pltpu.make_async_copy(cent_hbm, cent_rows, in_sem.at[3]),
    ]
    for load in loads:
        load.start()
    loads[0].wait()
    loads[1].wait()

    assigned = assigned_ref[...]
    high = lax.shift_right_logical(assigned, 7)
    low = jnp.bitwise_and(assigned, 127)
    table = table_ref[...]
    pick = one_hot(iota((T, L), 0) == high)
    looked = jnp.zeros((LANES, L), F32)
    shift = 0
    while 2**shift < O * S:
        digit = jnp.bitwise_and(lax.shift_right_logical(table, shift), 255)
        looked = looked + float(2**shift) * lax.dot_general(
            digit.astype(F32).astype(BF16), pick, (((0,), (0,)), ((), ())), preferred_element_type=F32
        )
        shift += 8
    slot = jnp.sum(jnp.where(iota((LANES, L), 0) == low, looked, 0.0), axis=0, keepdims=True)
    owner = jnp.floor((slot + 0.5) * (1.0 / S))
    row = jnp.floor((owner + 0.5) * (1.0 / C))
    owner_i = owner.astype(jnp.int32)
    row_i = row.astype(jnp.int32)
    cent_i = owner_i - row_i * C
    is_owner = jnp.where(iota((O, L), 0) == owner_i, 1.0, 0.0)
    is_row = jnp.where(iota((R, L), 0) == row_i, 1.0, 0.0)
    earlier = one_hot(iota((L, L), 0) < iota((L, L), 1))
    ranks = mm(jnp.concatenate([is_owner, is_row], axis=0).astype(BF16), earlier)
    rank_owner = jnp.sum(ranks[:O] * is_owner, axis=0, keepdims=True)
    rank_row = jnp.sum(ranks[O:] * is_row, axis=0, keepdims=True)
    block_i = jnp.bitwise_xor(row_i, row_me)
    if swap:
        block_i = jnp.where((block_i == 3) | (block_i == 4), 7 - block_i, block_i)
    position = block_i * Q + rank_row.astype(jnp.int32)
    rank_i = rank_owner.astype(jnp.int32)

    ahead = cent_i - col_me
    ahead = jnp.where(ahead < 0, ahead + C, ahead)
    behind = jnp.where(ahead == 0, 0, C - ahead)
    lane_i = behind * K + rank_i
    is_lane = one_hot(iota((LANES, L), 0) == lane_i)

    tag = slot - owner * S + 1.0
    tag_hi = jnp.floor(tag * (1.0 / 128.0))
    lines = jnp.concatenate(
        [(ahead * K + rank_i + 1).astype(F32), tag_hi, tag - tag_hi * 128.0, jnp.zeros((SUB - 3, L), F32)],
        axis=0,
    ).astype(BF16)

    def mark(t):
        here = jnp.where(position < (t + 1) * Q, position, -1)
        line = mm_t(lines, one_hot(iota((QP, L), 0) + t * Q == here))
        code_send[t, 0:1, :] = line[0:1]
        code_send[t, 1:2, :] = 128.0 * line[1:2] + line[2:3]

    each(0, R, mark)

    def cut(t, p):
        width = cuts[t][p] if small else D
        return pl.ds(sum(cuts[t][:p]) if small else 0, width), width

    def sem(t, p):
        return sum(len(c) for c in cuts[:t]) + p if small else t

    def pieces(t):
        return range(len(cuts[t])) if small else range(1)

    def ends(t, p):
        return int(direct and t == R - 1 and p >= len(cuts[t]) - straight)

    def row_copy(t, p):
        at = cut(t, p)[0]
        return remote(
            send_buf.at[t, :, at], chunk_buf.at[t, :, at], a_send.at[ends(t, p)], a_recv.at[sem(t, p) - 1], row_of(t), col_me
        )

    def code_group(t):
        return (0 if t == 1 else 2 if t == R - 1 else 1) if direct else t

    def code_copy(t):
        return remote(code_send.at[t], code_recv.at[t], m_send.at[0], m_recv.at[code_group(t)], row_of(t), col_me)

    def whole(ref, send, recv):
        return remote(ref, ref, send.at[0], recv.at[0], row_of(1), col_me)


    def start_rows(t):
        for p in pieces(t):
            if not ends(t, p):
                row_copy(t, p).start()

    def rows_at(t, block=0, count=None):
        return pl.ds(S + t * CK + block * K, CK if count is None else count)

    def dir_copy(d, p):
        at, width = cut(7, p)
        return remote(
            dir_buf.at[d, :, pl.ds((p - len(cuts[7]) + straight) * width, width)],
            all_buf.at[rows_at(7, (C - d) % C, K), at],
            d_send.at[0],
            f_recv.at[sem(7, p)],
            row_of(7),
            col_of[d],
        )

    def choose(ts):
        wanted = [one_hot(iota((Q, L), 0) + t * Q == position) for t in ts]
        found = mm(jnp.concatenate(wanted, axis=0), docs_ref[...]).astype(BF16)
        for i, t in enumerate(ts):
            send_buf[t] = found[i * Q : (i + 1) * Q]

    def first_sends():
        pl.semaphore_wait(barrier, R + C - 2)
        each(1, R, lambda t: code_copy(t).start())

    loads[2].wait()
    if R == 8:
        inner = lax.rem(bits[-1] + bits[-2], 2) == 1
        choose([3, 1])
        first_sends()

        @pl.when(inner)
        def _():
            start_rows(3)

        start_rows(1)
        choose([2, 4])
        start_rows(2)
        start_rows(4)

        @pl.when(jnp.logical_not(inner))
        def _():
            start_rows(3)

        choose([5, 6])
        start_rows(5)
        start_rows(6)
        choose([7, 0])
        start_rows(7)
        final = len(cuts[7]) - straight

        @pl.when(inner)
        def _():
            wanted = one_hot(iota((CK, L), 0) == jnp.where(block_i == 7, ahead * K + rank_i, -1))
            found = mm(wanted, docs_ref[:, D - tail :]).astype(BF16)
            dir_buf[...] = found.reshape(dir_buf.shape)

        @pl.when(jnp.logical_not(inner))
        def _():
            for p in range(final, len(cuts[7])):
                row_copy(7, p).start()
    else:
        first_sends()
        group = max(1, R // 2)
        for first in range(0, R, group):
            wanted = one_hot(iota((group * Q, L), 0) + first * Q == position)
            send_buf[first : first + group] = (
                mm(wanted, docs_ref[...]).astype(BF16).reshape(group, Q, D)
            )
            each(max(first, 1), first + group, start_rows)

    def fwd_copy(t, d, p):
        at = cut(t, p)[0]
        return remote(
            fwd_buf.at[t, d - 1, :, at],
            all_buf.at[rows_at(t, C - d, K), at],
            f_send.at[ends(t, p)],
            f_recv.at[sem(t, p)],
            row_me,
            col_of[d],
        )

    def fwd_arrival(t, p):
        ref = all_buf.at[rows_at(t, 1, CK - K), cut(t, p)[0]]
        return remote(ref, ref, f_send.at[0], f_recv.at[sem(t, p)], row_me, col_of[1])

    def tag_copy(t, d):
        return remote(
            tag_send.at[t], tag_recv.at[t, C - d], t_send.at[0], t_recv.at[t], row_me, col_of[d]
        )

    def tag_arrival(t):
        ref = tag_recv.at[t, pl.ds(1, C - 1)]
        return remote(ref, ref, t_send.at[0], t_recv.at[t], row_me, col_of[1])

    block = iota((CK, Q), 0) // K
    turned = jnp.where(block == 0, 0, C - block) * K + iota((CK, Q), 0) - block * K + 1

    def relay(t, p, mine=False):
        if ends(t, p):
            pl.when(jnp.logical_not(inner))(lambda: relay_now(t, p))
        else:
            relay_now(t, p, mine)

    def relay_now(t, p, mine=False):
        if not mine:
            if p == 0 and direct and t == R - 1:
                pl.when(jnp.logical_not(inner))(lambda: code_copy(t).wait_recv())
            elif p == 0 and not (direct and 1 < t < R - 1):
                code_copy(t).wait_recv()
            row_copy(t, p).wait_recv()
        at, width = cut(t, p)
        lines = (code_send if mine else code_recv)[t][:, :Q]
        line = lines[0:1].astype(jnp.int32)
        wanted = one_hot(iota((CK, Q), 0) + 1 == line)
        if p == 0:
            high = jnp.floor(lines[1:2] * (1.0 / 128.0))
            digits = [high, lines[1:2] - high * 128.0, jnp.zeros((SUB - 2, Q), F32)]
            digits = mm_t(jnp.concatenate(digits, axis=0).astype(BF16), one_hot(turned == line))
            tag_send[t, 0:1, :CK] = 128.0 * digits[0:1] + digits[1:2]
            for d in range(1, C):
                tag_copy(t, d).start()
        found = mm(wanted, (send_buf if mine else chunk_buf)[t, :, at]).astype(BF16)
        fwd_buf[t, :, :, at] = found[K:].reshape(C - 1, K, width)
        for d in range(1, C):
            fwd_copy(t, d, p).start()
        all_buf[rows_at(t, 0, K), at] = found[:K]

    if CK < LANES:
        tag_send[...] = jnp.zeros(tag_send.shape, F32)
    for p in pieces(0):
        relay(0, p, True)

    loads[3].wait()
    norm = jnp.zeros((S, LANES), F32)
    for part in range(0, D, LANES):
        block = all_buf[0:S, part : part + LANES].astype(F32)
        norm = norm + block * block
    cent_mat[...] = jnp.broadcast_to(
        lax.rsqrt(jnp.sum(norm, axis=1, keepdims=True) + 1.0), cent_mat.shape
    )


    eye = iota((CK, CK), 0) == iota((CK, CK), 1)

    def spread(t):
        tag_arrival(t).wait_recv()
        line = tag_send[t][:, :CK]
        for c in range(1, C):
            line = jnp.where(iota((1, CK), 1) // K == c, tag_recv[t, c][:, :CK], line)
        tag_row[t] = line
        tag_mat[t] = jnp.broadcast_to(
            jnp.sum(jnp.where(eye, line, 0.0), axis=1, keepdims=True), (CK, CK)
        )
        best_mat[t] = jnp.zeros((CK, CK), F32)

    stats_ref[...] = jnp.zeros(stats_ref.shape, F32)

    def member_of(t):
        return (iota((S, CK), 0) + 1).astype(F32) == tag_row[t]

    def self_block(t, gram):
        diag = jnp.where(eye, gram, 0.0)
        row_scale = lax.rsqrt(jnp.sum(diag, axis=0, keepdims=True) + 1.0)
        col_scale = lax.rsqrt(jnp.sum(diag, axis=1, keepdims=True) + 1.0)
        inv_row[t] = row_scale
        inv_mat[t] = jnp.broadcast_to(col_scale, (CK, CK))
        line = jnp.where(tag_row[t] > 0.0, tag_row[t], -1.0)
        same = (tag_mat[t] == line) & jnp.logical_not(eye)
        best = jnp.max(jnp.where(same, gram * col_scale, 0.0), axis=0, keepdims=True)
        return row_scale, line, best

    def other_block(u, gram, row_scale, line, best):
        same = tag_mat[u] == line
        best_mat[u] = jnp.maximum(best_mat[u], jnp.where(same, gram * row_scale, 0.0))
        return jnp.maximum(
            best, jnp.max(jnp.where(same, gram * inv_mat[u], 0.0), axis=0, keepdims=True)
        )

    def cross_block(t, cross, row_scale):
        member = member_of(t)
        similarity = row_scale * jnp.sum(
            jnp.where(member, cross * cent_mat[...], 0.0), axis=0, keepdims=True
        )
        sim_row[t] = similarity
        lines = [jnp.ones((1, CK), BF16), *split3(similarity), *split3(similarity * similarity)]
        lines = jnp.concatenate(
            [line.astype(F32) for line in lines] + [jnp.zeros((1, CK), F32)], axis=0
        )
        stats_ref[...] += mm_t(lines.astype(BF16), one_hot(member))

    def settle(t, read):
        row_scale, line, best = self_block(t, read(S + t * CK, CK))
        for u in range(t):
            best = other_block(u, read(S + u * CK, CK), row_scale, line, best)
        best_row[t] = best
        cross_block(t, read(0, S), row_scale)

    def arrivals(t, p):
        fwd_arrival(t, p).wait_recv()

    def absorb_piece(t, p):
        if p == 0:
            spread(t)
        arrivals(t, p)
        at = cut(t, p)[0]
        rows = S + (t + 1) * CK
        before = gram_acc[0:rows] if p else None
        part = mm_t(all_buf[0:rows, at], all_buf[rows_at(t), at])
        gram_acc[0:rows] = part if p == 0 else before + part
        if p == len(cuts[t]) - 1:
            settle(t, lambda start, count: gram_acc[start : start + count])

    def absorb_loop(t):
        n = len(cuts[t])
        width = cuts[t][0]
        rows = S + (t + 1) * CK
        first_straight = n - straight if t == R - 1 else n
        slow = first_straight - 1
        spread(t)

        def step(i, carry):
            p = i
            if first_straight < n:
                ahead_of = jnp.logical_and(i >= slow, i < n - 2)
                p = jnp.where(i == n - 2, slow, i + jnp.where(ahead_of, 1, 0))
            at = pl.ds(pl.multiple_of(p * width, width), width)
            semaphore = f_recv.at[sem(t, 0) + p]

            def relayed():
                ref = all_buf.at[rows_at(t, 1, CK - K), at]
                remote(ref, ref, d_send.at[0], semaphore, row_me, col_of[1]).wait_recv()

            if first_straight < n:

                @pl.when(jnp.logical_and(inner, p >= first_straight))
                def _():
                    ref = all_buf.at[rows_at(t), at]
                    remote(ref, ref, d_send.at[0], semaphore, row_me, col_of[1]).wait_recv()

                pl.when(jnp.logical_or(jnp.logical_not(inner), p < first_straight))(relayed)
            else:
                relayed()
            before = jnp.where(i > 0, gram_acc[0:rows], 0.0)
            gram_acc[0:rows] = before + mm_t(all_buf[0:rows, at], all_buf[rows_at(t), at])
            return carry

        lax.fori_loop(0, n, step, 0)
        settle(t, lambda start, count: gram_acc[start : start + count])

    def absorb(t):
        for p in pieces(t):
            absorb_piece(t, p)

    def absorb_any(t):
        spread(t)
        arrivals(t, 0)
        mine = all_buf[rows_at(t), :]
        row_scale, line, best = self_block(t, mm_t(mine, mine))

        def pair(u, best):
            return other_block(u, mm_t(all_buf[rows_at(u), :], mine), row_scale, line, best)

        best_row[t] = lax.fori_loop(0, t, pair, best)
        cross_block(t, mm_t(all_buf[0:S, :], mine), row_scale)

    def relay_all(*ts):
        for p in pieces(ts[0]):
            for t in ts:
                relay(t, p)

    if R == 8:
        relay_all(1)

        @pl.when(inner)
        def _():
            code_copy(7).wait_recv()
            for p in range(len(cuts[7]) - straight, len(cuts[7])):
                for d in range(C):
                    dir_copy(d, p).start()

        absorb(0)
        ref = code_recv.at[pl.ds(2, R - 3)]
        remote(ref, ref, m_send.at[0], m_recv.at[1], row_of(1), col_me).wait_recv()

        @pl.when(inner)
        def _():
            relay_all(2, 3)

        @pl.when(jnp.logical_not(inner))
        def _():
            relay_all(3, 2)

        absorb(1)
        relay(4, 0)
        relay(5, 0)
        absorb(2)
        relay(4, 1)
        relay(5, 1)
        absorb(3)
        absorb(4)
        absorb(5)
        relay_all(6)
        relay_all(7)
        absorb_loop(6)
        absorb_loop(R - 1)
    elif small:
        for t in range(1, R):
            relay_all(t)
            absorb(t - 1)
        absorb(R - 1)
    else:

        def advance(t, carry):
            relay_all(t)
            absorb_any(t - 1)
            return carry

        lax.fori_loop(1, R, advance, 0)
        absorb_any(R - 1)

    stats = stats_ref[...]
    count = stats[0:1]
    total = stats[1:2] + stats[2:3] + stats[3:4]
    square = stats[4:5] + stats[5:6] + stats[6:7]
    share = 1.0 / jnp.maximum(count, 1.0)
    mean = total * share
    variance = jnp.maximum(square * share - mean * mean, 0.0)
    spread_inv = lax.rsqrt(variance + 1.0 / D)
    wanted = [line.astype(F32) for line in (*split3(mean), *split3(spread_inv))]
    wanted = jnp.concatenate(wanted + [jnp.zeros((2, S), F32)], axis=0).astype(BF16)

    def res_copy(t, r, d):
        return remote(
            res_send.at[t], res_recv.at[t * C + (C - d) % C], r_send.at[0], r_recv.at[0], r, col_of[d]
        )

    res_all = whole(res_recv.at[pl.ds(1, O - 1)], r_send, r_recv)

    def finish(t, found):
        centre = found[0:1] + found[1:2] + found[2:3]
        width = found[3:4] + found[4:5] + found[5:6]
        proto = (centre - sim_row[t]) * width
        column = jnp.max(best_mat[t], axis=1, keepdims=True)
        flat = jnp.max(jnp.where(eye, column, 0.0), axis=0, keepdims=True)
        redundant = jnp.maximum(flat, best_row[t]) * inv_row[t] * math.sqrt(D)
        res_send[t, 0:1, :CK] = proto
        res_send[t, 1:2, :CK] = redundant

    if CK < LANES:
        res_send[...] = jnp.zeros(res_send.shape, F32)

    def deliver(t):
        r = row_of(t)
        for d in (2, 3, 1, 0) if C == 4 else range(C):
            if not (isinstance(t, int) and t == 0 and d == 0):
                res_copy(t, r, d).start()

    if small:
        members = jnp.concatenate([one_hot(member_of(t)) for t in range(R)], axis=1)
        found = mm(wanted, members)
        for t in range(R):
            finish(t, found[:, t * CK : (t + 1) * CK])
        for t in [5, 3, 4, 2, 7, 6, 1, 0] if R == 8 else range(R):
            deliver(t)
    else:

        def finish_any(t):
            finish(t, mm(wanted, one_hot(member_of(t))))

        each(0, R, finish_any)
        each(1, R, deliver)
        deliver(0)
    res_recv[0] = res_send[0]
    out_ref[2:3, :S] = count
    out_ref[3:4, :S] = total
    out_ref[4:5, :S] = square

    def sent(ref, semaphore):
        remote(ref, ref, semaphore, r_recv.at[0], row_me, col_of[1]).wait_send()

    if direct:
        kept = D - tail
        sent(send_buf.at[pl.ds(1, R - 2)], a_send.at[0])
        sent(send_buf.at[R - 1, :, pl.ds(0, kept)], a_send.at[0])
        sent(fwd_buf.at[pl.ds(0, R - 1)], f_send.at[0])
        sent(fwd_buf.at[R - 1, :, :, pl.ds(0, kept)], f_send.at[0])

        @pl.when(inner)
        def _():
            sent(dir_buf, d_send.at[0])

        @pl.when(jnp.logical_not(inner))
        def _():
            sent(send_buf.at[R - 1, :, pl.ds(kept, D - kept)], a_send.at[1])
            sent(fwd_buf.at[R - 1, :, :, pl.ds(kept, D - kept)], f_send.at[1])

    else:
        sent(send_buf.at[pl.ds(1, R - 1)], a_send.at[0])
        sent(fwd_buf, f_send.at[0])
    sent(code_recv.at[pl.ds(1, R - 1)], m_send.at[0])
    sent(tag_recv.at[:, pl.ds(1, C - 1)], t_send.at[0])
    res_all.wait_send()
    res_all.wait_recv()

    for o in range(O):
        pair = res_recv[o]
        res_rows[o : o + 1, :] = pair[0:1]
        res_rows[O + o : O + o + 1, :] = pair[1:2]
    parts = jnp.concatenate([line.astype(F32) for line in split3(res_rows[...])], axis=0)
    found = mm(parts.astype(BF16), is_lane)
    found = found[: 2 * O] + found[2 * O : 4 * O] + found[4 * O :]
    mask = iota((O, L), 0) == block_i * C + ahead
    out_ref[0:1, :L] = jnp.sum(jnp.where(mask, found[:O], 0.0), axis=0, keepdims=True)
    out_ref[1:2, :L] = jnp.sum(jnp.where(mask, found[O:], 0.0), axis=0, keepdims=True)


def local(documents, assigned, centroids, owner_slot):
    L, D = documents.shape
    S = centroids.shape[0]
    R = lax.axis_size("dp")
    C = lax.axis_size("cent")
    O = R * C
    pair_cap = 2 * L // O
    row_cap = 5 * C * pair_cap // 8
    K = round_up(pair_cap, 16)
    Q = round_up(row_cap, 16)
    CK = C * K
    QP = round_up(Q, LANES)
    half, unit = D // 2, D // 8
    cuts = [(D,)] + [(half, half)] * (R - 3) + [(2 * unit,) * 4, (2 * unit,) * 4]
    straight = 2
    copies = sum(len(c) for c in cuts) if R <= 8 else R
    T = owner_slot.shape[0] // LANES
    hbm = pl.BlockSpec(memory_space=pl.ANY)
    dma = pltpu.SemaphoreType.DMA
    packed = pl.pallas_call(
        functools.partial(kernel, (R, C, K, Q, cuts, straight)),
        name="cluster_exchange",
        out_shape=pltpu.VMEM((SUB, max(L, S)), F32),
        in_specs=[hbm] * 4,
        out_specs=pl.BlockSpec(memory_space=pltpu.VMEM),
        scratch_shapes=[
            pltpu.VMEM((L, D), BF16),
            pltpu.VMEM((1, L), jnp.int32),
            pltpu.VMEM((T, LANES), jnp.int32),
            pltpu.VMEM((S + R * CK, D), BF16),
            pltpu.VMEM((R, Q, D), BF16),
            pltpu.VMEM((R, Q, D), BF16),
            pltpu.VMEM((R, 2, QP), F32),
            pltpu.VMEM((R, 2, QP), F32),
            pltpu.VMEM((R, C - 1, K, D), BF16),
            pltpu.VMEM((C, K, straight * cuts[-1][-1]), BF16),
            pltpu.VMEM((R, 1, LANES), F32),
            pltpu.VMEM((R, C, 1, LANES), F32),
            pltpu.VMEM((R, 2, LANES), F32),
            pltpu.VMEM((O, 2, LANES), F32),
            pltpu.VMEM((2 * O, LANES), F32),
            pltpu.VMEM((R, 1, CK), F32),
            pltpu.VMEM((R, CK, CK), F32),
            pltpu.VMEM((R, 1, CK), F32),
            pltpu.VMEM((R, CK, CK), F32),
            pltpu.VMEM((R, 1, CK), F32),
            pltpu.VMEM((R, 1, CK), F32),
            pltpu.VMEM((R, CK, CK), F32),
            pltpu.VMEM((S, CK), F32),
            pltpu.VMEM((S + R * CK if R <= 8 else SUB, CK), F32),
            pltpu.VMEM((SUB, S), F32),
            dma((4,)),
            dma((2,)),
            dma((copies - 1,)),
            dma((1,)),
            dma((3 if R == 8 else R,)),
            dma((2,)),
            dma((copies,)),
            dma((1,)),
            dma((R,)),
            dma((1,)),
            dma((1,)),
            dma((1,)),
        ],
        compiler_params=pltpu.CompilerParams(
            collective_id=0, has_side_effects=True, vmem_limit_bytes=62 * 1024 * 1024
        ),
    )(
        documents,
        assigned.reshape(1, L),
        centroids,
        owner_slot.reshape(-1, LANES),
    )

    def spill(packed_ref, proto_ref, red_ref, stats_ref, sems):
        copies = [
            pltpu.make_async_copy(packed_ref.at[pl.ds(0, 1), pl.ds(0, L)], proto_ref, sems.at[0]),
            pltpu.make_async_copy(packed_ref.at[pl.ds(1, 1), pl.ds(0, L)], red_ref, sems.at[1]),
            pltpu.make_async_copy(packed_ref.at[pl.ds(2, 3), pl.ds(0, S)], stats_ref, sems.at[2]),
        ]
        for copy in copies:
            copy.start()
        for copy in copies:
            copy.wait()

    proto, red, stats = pl.pallas_call(
        spill,
        name="spill",
        out_shape=[jax.ShapeDtypeStruct((1, L), F32)] * 2 + [jax.ShapeDtypeStruct((3, S), F32)],
        in_specs=[pl.BlockSpec(memory_space=pltpu.VMEM)],
        out_specs=[hbm] * 3,
        scratch_shapes=[dma((3,))],
    )(pltpu.with_memory_space_constraint(packed, pltpu.VMEM))
    return proto.reshape(L), red.reshape(L), stats


def solution(mesh):
    in_specs = (P(("dp", "cent"), None), P(("dp", "cent")), P(("dp", "cent"), None), P())
    out_specs = (P(("dp", "cent")), P(("dp", "cent")), P(None, ("dp", "cent")))
    return jax.shard_map(local, mesh=mesh, in_specs=in_specs, out_specs=out_specs, check_vma=False)
```
